32 devices in a mesh: rep: 4 (over x, y), dp: 8 (over z, core).
Axes of the slice: x: 2, y: 2, z: 4, core: 2. Of those that a mesh axis runs over, the one named last changes fastest.
Arguments:
- x: bfloat16 [32, 4096, 512], P(('rep', 'dp')), parts along dimension 0
- dy: bfloat16 [32, 4096, 512], P(('rep', 'dp')), parts along dimension 0
- w_gate: bfloat16 [2, 512, 1408], P(None, 'dp')
- w_up: bfloat16 [2, 512, 1408], P(None, 'dp')
- w_down: bfloat16 [2, 1408, 512], P(None, 'dp')
Outputs:
- output 1: bfloat16 [32, 4096, 512], P(('rep', 'dp')), parts along dimension 0
- output 2: bfloat16 [8, 512, 1408], P('rep', 'dp'), parts along dimension 0
- output 3: bfloat16 [8, 512, 1408], P('rep', 'dp'), parts along dimension 0
- output 4: bfloat16 [8, 1408, 512], P('rep', 'dp'), parts along dimension 0
There are 4 independent parts. The reference program is written for one: setup_inputs(seed, part) draws one part's arguments, and reference() takes and returns one part's arrays. A program takes and returns all parts, laid end to end along the dimension named above; an argument that names none is the same for every part.
All inputs are finite; a program needn't handle non-finite values.
Results may differ from the reference program's by a relative error of at most 0.018.
Values are sent between devices in bfloat16 or wider.
A program may use at most 2 GiB of HBM per device.

```python
import jax
import jax.numpy as jnp
from jax import lax

SEQUENCES = 8
TOKENS = 4096
D = 512
FF = 1408
LAYERS = 2
NAMES = ("w_gate", "w_up", "w_down")
SHAPES = {"w_gate": (LAYERS, D, FF), "w_up": (LAYERS, D, FF), "w_down": (LAYERS, FF, D)}


def bump(key, n, height):
    away = (jnp.arange(n, dtype=jnp.int32) - jax.random.randint(key, (), 0, n, jnp.int32)) % n
    return jnp.where(away < n // 8, height, 1.0)


def together(key, own, strength):
    shared = jax.random.normal(key, own.shape[1:], jnp.float32)
    return (own + strength * shared) * lax.rsqrt(1 + strength * strength)


def setup_inputs(seed: int = 0, part: int = 0) -> dict:
    kx, kdy, ka, kb, kz, kf, kh, kl, *kw = jax.random.split(jax.random.key(seed), 8 + len(NAMES))
    kx, kdy, ka, kb = (jax.random.fold_in(k, part) for k in (kx, kdy, ka, kb))
    shape = (SEQUENCES, TOKENS, D)
    much_x, much_dy = jax.random.uniform(kz, (2,), jnp.float32, 0.0, 1.0)
    layers = 2.0 ** jax.random.uniform(kl, (LAYERS, 1, 1), jnp.float32, -1.0, 1.0)
    x = together(ka, jax.random.normal(kx, shape, jnp.float32), much_x) * bump(kf, D, 4.0)
    dy = together(kb, jax.random.normal(kdy, shape, jnp.float32), much_dy)
    drawn = {"x": x.astype(jnp.bfloat16), "dy": (dy * (SEQUENCES * TOKENS) ** -0.5).astype(jnp.bfloat16)}
    for key, name in zip(kw, NAMES, strict=True):
        w = jax.random.normal(key, SHAPES[name], jnp.float32) * SHAPES[name][1] ** -0.5
        drawn[name] = (w * {"w_gate": 1.0, "w_up": bump(kh, FF, 4.0), "w_down": layers}[name]).astype(jnp.bfloat16)
    return drawn


def matmul(a, w):
    return jnp.dot(a, w, preferred_element_type=jnp.float32).astype(jnp.bfloat16)


def normed(h):
    wide = h.astype(jnp.float32)
    scale = lax.rsqrt(jnp.mean(wide**2, -1, keepdims=True) + 1e-6)
    return (wide * scale).astype(jnp.bfloat16)


def layer(h, w):
    a = normed(h)
    gate = jnp.dot(a, w["w_gate"], preferred_element_type=jnp.float32)
    up = jnp.dot(a, w["w_up"], preferred_element_type=jnp.float32)
    return h + matmul((jax.nn.silu(gate) * up).astype(jnp.bfloat16), w["w_down"])


def stack(weights, h):
    return lax.scan(lambda h, w: (layer(h, w), None), h, weights)[0]


def reference(x, dy, w_gate, w_up, w_down):
    weights = dict(zip(NAMES, (w_gate, w_up, w_down), strict=True))

    def take(so_far, sequence):
        h, by_y = sequence
        _, back = jax.vjp(stack, weights, h)
        by_weights, by_h = back(by_y)
        return jax.tree.map(lambda total, term: total + term.astype(jnp.float32), so_far, by_weights), by_h

    none_yet = {name: jnp.zeros(w.shape, jnp.float32) for name, w in weights.items()}
    by_weights, by_x = lax.scan(take, none_yet, (x, dy))
    return (by_x, *(by_weights[name].astype(jnp.bfloat16) for name in NAMES))
```

```python
import jax
import jax.numpy as jnp
from jax import lax
from jax.sharding import PartitionSpec as P

EPS = 1e-6


def dot(a, b, dims):
    return lax.dot_general(a, b, (dims, ((), ())), preferred_element_type=jnp.float32)


NN, NT, TN = ((1,), (0,)), ((1,), (1,)), ((0,), (0,))


def normed(h):
    wide = h.astype(jnp.float32)
    scale = lax.rsqrt(jnp.mean(wide**2, -1, keepdims=True) + EPS)
    return (wide * scale).astype(jnp.bfloat16), scale


def gather(w):
    return lax.all_gather(w, "dp", axis=0, tiled=True)


def scatter(g):
    return lax.psum_scatter(g.astype(jnp.bfloat16), "dp", scatter_dimension=0, tiled=True)


def solution(mesh):
    def step(x, dy, w_gate, w_up, w_down):
        x, dy = x[0], dy[0]
        layers = w_gate.shape[0]
        ff = w_gate.shape[2]
        w1 = [gather(jnp.concatenate([w_gate[n], w_up[n]], axis=1)) for n in range(layers)]
        w2 = [gather(w_down[n]) for n in range(layers)]
        states = [x]
        for n in range(layers - 1):
            a, _ = normed(states[-1])
            gu = dot(a, w1[n], NN)
            p = (jax.nn.silu(gu[:, :ff]) * gu[:, ff:]).astype(jnp.bfloat16)
            states.append(states[-1] + dot(p, w2[n], NN).astype(jnp.bfloat16))
        out = dy
        by1, by2 = [None] * layers, [None] * layers
        for n in reversed(range(layers)):
            h = states[n]
            a, scale = normed(h)
            gu = dot(a, w1[n], NN)
            gate, up = gu[:, :ff], gu[:, ff:]
            s = jax.nn.sigmoid(gate)
            silu = gate * s
            p = (silu * up).astype(jnp.bfloat16)
            by2[n] = scatter(dot(p, out, TN))
            dp = dot(out, w2[n], NT).astype(jnp.bfloat16).astype(jnp.float32)
            dgu = jnp.concatenate([dp * up * (s + silu * (1 - s)), dp * silu], axis=1).astype(jnp.bfloat16)
            by1[n] = scatter(dot(a, dgu, TN))
            da = dot(dgu, w1[n], NT).astype(jnp.bfloat16).astype(jnp.float32)
            wide = h.astype(jnp.float32)
            inner = jnp.mean(da * wide, -1, keepdims=True)
            dh = scale * da - (scale * scale * scale * inner) * wide
            out = out + dh.astype(jnp.bfloat16)
        by1, by2 = jnp.stack(by1), jnp.stack(by2)
        return out[None], by1[:, :, :ff], by1[:, :, ff:], by2

    whole, rows = P(("rep", "dp"), None, None), P(None, "dp", None)
    group = P("rep", "dp", None)
    return jax.shard_map(step, mesh=mesh, in_specs=(whole, whole, rows, rows, rows), out_specs=(whole, group, group, group), check_vma=False)
```

```python
import functools

import jax
import jax.numpy as jnp
from jax import lax
from jax.experimental import pallas as pl
from jax.experimental.pallas import tpu as pltpu
from jax.sharding import PartitionSpec as P

EPS = 1e-6
BF, F32 = jnp.bfloat16, jnp.float32
TM = 512
CH = 256
VMEM_LIMIT = 60 * 2**20


def dot(a, b):
    return jnp.dot(a, b, preferred_element_type=F32)


def dot_nt(a, b):
    return lax.dot_general(a, b, (((1,), (1,)), ((), ())), preferred_element_type=F32)


def chunks(ff):
    return [(s, min(CH, ff - s)) for s in range(0, ff, CH)]


def joined(gate, up):
    return jnp.concatenate([t[:, s : s + w] for s, w in chunks(gate.shape[1]) for t in (gate, up)], axis=1)


def parted(t):
    ff = t.shape[1] // 2
    gate = jnp.concatenate([t[:, 2 * s : 2 * s + w] for s, w in chunks(ff)], axis=1)
    up = jnp.concatenate([t[:, 2 * s + w : 2 * (s + w)] for s, w in chunks(ff)], axis=1)
    return gate, up


def scale_of(wide):
    return lax.rsqrt(jnp.mean(wide * wide, -1, keepdims=True) + EPS)


def sigmoid(t):
    return 0.5 * jnp.tanh(0.5 * t) + 0.5


def forward_kernel(h_ref, w1_ref, w2_ref, o_ref, p_ref):
    ff = w2_ref.shape[0]
    wide = h_ref[...].astype(F32)
    a = (wide * scale_of(wide)).astype(BF)
    for s, w in chunks(ff):
        gu = dot(a, w1_ref[:, 2 * s : 2 * (s + w)])
        gate, up = gu[:, :w], gu[:, w:]
        p_ref[:, s : s + w] = (gate * sigmoid(gate) * up).astype(BF)
    o_ref[...] = h_ref[...] + dot(p_ref[...], w2_ref[...]).astype(BF)


def hidden_kernel(h_ref, by_ref, w1_ref, w2_ref, dgu_ref, at_ref, dw2_ref, p_ref, acc_ref):
    ff = w2_ref.shape[0]
    step = pl.program_id(0)
    wide = h_ref[...].astype(F32)
    a = (wide * scale_of(wide)).astype(BF)
    at_ref[...] = a.T
    by = by_ref[...]
    for s, w in chunks(ff):
        gu = dot(a, w1_ref[:, 2 * s : 2 * (s + w)])
        dp = dot_nt(by, w2_ref[s : s + w, :]).astype(BF).astype(F32)
        gate, up = gu[:, :w], gu[:, w:]
        sg = sigmoid(gate)
        silu = gate * sg
        p_ref[:, s : s + w] = (silu * up).astype(BF)
        dgu_ref[:, 2 * s : 2 * s + w] = (dp * up * (sg + silu * (1 - sg))).astype(BF)
        dgu_ref[:, 2 * s + w : 2 * (s + w)] = (dp * silu).astype(BF)
    term = dot(by.T, p_ref[...])

    @pl.when(step == 0)
    def _():
        acc_ref[...] = term

    @pl.when(step > 0)
    def _():
        acc_ref[...] += term

    @pl.when(step == pl.num_programs(0) - 1)
    def _():
        dw2_ref[...] = acc_ref[...].astype(BF).T


def weights_kernel(at_ref, dgu_ref, dw1_ref):
    dw1_ref[...] = dot(at_ref[...], dgu_ref[...]).astype(BF)


def input_kernel(h_ref, by_ref, dgu_ref, w1_ref, o_ref):
    da = dot_nt(dgu_ref[...], w1_ref[...]).astype(BF).astype(F32)
    wide = h_ref[...].astype(F32)
    scale = scale_of(wide)
    inner = jnp.mean(da * wide, -1, keepdims=True)
    o_ref[...] = by_ref[...] + (scale * da - (scale * scale * scale * inner) * wide).astype(BF)


def params():
    return pltpu.CompilerParams(dimension_semantics=("arbitrary",), vmem_limit_bytes=VMEM_LIMIT)


def cost(flops, nbytes):
    return pl.CostEstimate(flops=flops, bytes_accessed=nbytes, transcendentals=0)


def whole(shape):
    return pl.BlockSpec(shape, lambda i: (0,) * len(shape))


def rows(width):
    return pl.BlockSpec((TM, width), lambda i: (i, 0))


def forward(h, w1, w2):
    t, d = h.shape
    ff = w2.shape[0]
    return pl.pallas_call(
        forward_kernel, grid=(t // TM,), name="forward",
        in_specs=[rows(d), whole(w1.shape), whole(w2.shape)], out_specs=rows(d),
        out_shape=jax.ShapeDtypeStruct((t, d), BF), scratch_shapes=[pltpu.VMEM((TM, ff), BF)],
        compiler_params=params(), cost_estimate=cost(6 * t * d * ff, 4 * t * d),
    )(h, w1, w2)


def hidden(h, by, w1, w2):
    t, d = h.shape
    ff = w2.shape[0]
    return pl.pallas_call(
        hidden_kernel, grid=(t // TM,), name="hidden",
        in_specs=[rows(d), rows(d), whole(w1.shape), whole(w2.shape)],
        out_specs=[rows(2 * ff), pl.BlockSpec((d, TM), lambda i: (0, i)), whole((ff, d))],
        out_shape=[jax.ShapeDtypeStruct(s, BF) for s in ((t, 2 * ff), (d, t), (ff, d))],
        scratch_shapes=[pltpu.VMEM((TM, ff), BF), pltpu.VMEM((d, ff), F32)],
        compiler_params=params(), cost_estimate=cost(8 * t * d * ff, 8 * t * d + 4 * t * ff),
    )(h, by, w1, w2)


def by_weights(at, dgu):
    d, t = at.shape
    n = dgu.shape[1]
    return pl.pallas_call(
        weights_kernel, grid=(n // 256,), name="by_weights",
        in_specs=[whole((d, t)), pl.BlockSpec((t, 256), lambda i: (0, i))],
        out_specs=pl.BlockSpec((d, 256), lambda i: (0, i)),
        out_shape=jax.ShapeDtypeStruct((d, n), BF),
        compiler_params=params(), cost_estimate=cost(2 * t * d * n, 2 * t * n + 2 * t * d),
    )(at, dgu)


def by_input(h, by, dgu, w1):
    t, d = h.shape
    n = dgu.shape[1]
    return pl.pallas_call(
        input_kernel, grid=(t // TM,), name="by_input",
        in_specs=[rows(d), rows(d), rows(n), whole(w1.shape)], out_specs=rows(d),
        out_shape=jax.ShapeDtypeStruct((t, d), BF),
        compiler_params=params(), cost_estimate=cost(2 * t * d * n, 2 * t * n + 6 * t * d),
    )(h, by, dgu, w1)


def gather(w):
    return lax.all_gather(w, "dp", axis=0, tiled=True)


def scatter(g):
    return lax.psum_scatter(g, "dp", scatter_dimension=0, tiled=True)


def solution(mesh):
    def step(x, dy, w_gate, w_up, w_down):
        x, by = x[0], dy[0]
        layers = w_gate.shape[0]
        w1 = [gather(joined(w_gate[n], w_up[n])) for n in range(layers)]
        w2 = [gather(w_down[n]) for n in range(layers)]
        states = [x]
        for n in range(layers - 1):
            states.append(forward(states[-1], w1[n], w2[n]))
        g1, g2 = [None] * layers, [None] * layers
        for n in reversed(range(layers)):
            dgu, at, dw2 = hidden(states[n], by, w1[n], w2[n])
            g2[n] = scatter(dw2)
            g1[n] = scatter(by_weights(at, dgu))
            by = by_input(states[n], by, dgu, w1[n])
        gates, ups = zip(*(parted(g) for g in g1))
        return by[None], jnp.stack(gates), jnp.stack(ups), jnp.stack(g2)

    spread, by_rows = P(("rep", "dp"), None, None), P(None, "dp", None)
    group = P("rep", "dp", None)
    return jax.shard_map(
        step, mesh=mesh, in_specs=(spread, spread, by_rows, by_rows, by_rows),
        out_specs=(spread, group, group, group), check_vma=False,
    )
```

```python
import functools

import jax
import jax.numpy as jnp
from jax import lax
from jax.experimental import pallas as pl
from jax.experimental.pallas import tpu as pltpu
from jax.sharding import PartitionSpec as P

EPS = 1e-6
BF, F32 = jnp.bfloat16, jnp.float32
TM = 512
CH = 256
VMEM_LIMIT = 60 * 2**20


def dot(a, b):
    return jnp.dot(a, b, preferred_element_type=F32)


def dot_nt(a, b):
    return lax.dot_general(a, b, (((1,), (1,)), ((), ())), preferred_element_type=F32)


def chunks(ff):
    return [(s, min(CH, ff - s)) for s in range(0, ff, CH)]


def joined(gate, up):
    return jnp.concatenate([t[:, s : s + w] for s, w in chunks(gate.shape[1]) for t in (gate, up)], axis=1)


def parted(t):
    ff = t.shape[1] // 2
    gate = jnp.concatenate([t[:, 2 * s : 2 * s + w] for s, w in chunks(ff)], axis=1)
    up = jnp.concatenate([t[:, 2 * s + w : 2 * (s + w)] for s, w in chunks(ff)], axis=1)
    return gate, up


def scale_of(wide):
    return lax.rsqrt(jnp.mean(wide * wide, -1, keepdims=True) + EPS)


def sigmoid(t):
    return 0.5 * jnp.tanh(0.5 * t) + 0.5


MESH = pl.DeviceIdType.MESH
Z = 4


def place():
    dp = lax.axis_index("dp")
    return lax.axis_index("rep"), dp // 2, dp % 2


def remote(src, dst, send, recv, rep, z, core):
    return pltpu.make_async_remote_copy(src_ref=src, dst_ref=dst, send_sem=send, recv_sem=recv, device_id=(rep, 2 * z + core), device_id_type=MESH)


def meet(peers):
    barrier = pltpu.get_barrier_semaphore()
    for rep, z, core in peers:
        pl.semaphore_signal(barrier, inc=1, device_id=(rep, 2 * z + core), device_id_type=MESH)
    pl.semaphore_wait(barrier, len(peers))


def z_peers():
    rep, z, core = place()
    return [(rep, (z + i) % Z, core) for i in range(1, Z)]


def rep_peers():
    rep, z, core = place()
    return [((rep + i) % 4, z, core) for i in range(1, 4)]


def sibling():
    rep, z, core = place()
    return rep, z, 1 - core


class Gather:
    SEMS = 3 + 9 + 13

    def __init__(self, gate, up, down, w1, w2, shard, sems):
        self.gate, self.up, self.down, self.w1, self.w2, self.shard, self.sems = gate, up, down, w1, w2, shard, sems
        self.local_sems, self.send_sems, self.recv_sems = sems
        self.r1, self.r2 = gate.shape[1], down.shape[1]
        self.cols = w2.shape[1] // 4

    def block(self, z, core):
        s = 2 * z + core
        return (
            self.w1.at[pl.ds(pl.multiple_of(s * self.r1, self.r1), self.r1), :],
            self.w2.at[pl.ds(pl.multiple_of(s * self.r2, self.r2), self.r2), :],
        )

    def quarter(self, z, core, q):
        s, n = 2 * z + core, self.r1 // 4
        return (
            self.w1.at[pl.ds(pl.multiple_of(s * self.r1 + q * n, n), n), :],
            self.w2.at[pl.ds(pl.multiple_of(s * self.r2, self.r2), self.r2), pl.ds(pl.multiple_of(q * self.cols, self.cols), self.cols)],
        )

    def copies(self, number, srcs, dsts, to):
        return [remote(s, d, self.send_sems.at[2 * number + i], self.recv_sems.at[2 * number + i], *to) for i, (s, d) in enumerate(zip(srcs, dsts))]

    def along_z(self, i):
        rep, z, core = place()
        n = self.r1 // 4
        own = (self.shard.at[pl.ds(pl.multiple_of(rep * n, n), n), :], self.down.at[0, :, pl.ds(pl.multiple_of(rep * self.cols, self.cols), self.cols)])
        return self.copies(i - 1, own, self.quarter(z, core, rep), (rep, (z + i) % Z, core))

    def across(self, i, j):
        rep, z, core = place()
        part = self.quarter((z + Z - i) % Z, core, rep)
        return self.copies(3 + 3 * (i - 1) + j - 1, part, part, ((rep + j) % 4, z, core))

    def inside(self, i, j):
        rep, z, core = place()
        part = self.quarter((z + Z - i) % Z, core, (rep + 4 - j) % 4)
        return self.copies(13 + 4 * (i - 1) + j, part, part, sibling())

    def inside_own(self):
        _, z, core = place()
        return self.copies(12, (self.shard, self.down.at[0]), self.block(z, core), sibling())

    def keep_own(self):
        _, z, core = place()
        return [pltpu.make_async_copy(s, d, self.local_sems.at[i]) for i, (s, d) in enumerate(zip((self.shard, self.down.at[0]), self.block(z, core)))]

    def join(self):
        for s, w in chunks(self.gate.shape[2]):
            self.shard[:, 2 * s : 2 * s + w] = self.gate[0, :, s : s + w]
            self.shard[:, 2 * s + w : 2 * (s + w)] = self.up[0, :, s : s + w]

    def begin(self):
        meet(z_peers() + rep_peers() + [sibling()])
        for i in (2, 1, 3):
            for c in self.along_z(i):
                c.start()
        for c in self.inside_own() + self.keep_own():
            c.start()

    def hand_on(self, i):
        for c in self.along_z(i):
            c.wait_recv()
        for j in range(1, 4):
            for c in self.across(i, j):
                c.start()
        for c in self.inside(i, 0):
            c.start()

    def pass_in(self, i):
        for j in range(1, 4):
            for c in self.across(i, j):
                c.wait_recv()
            for c in self.inside(i, j):
                c.start()

    def end(self):
        for c in self.inside_own():
            c.wait()
        for i in range(1, Z):
            for c in self.along_z(i):
                c.wait_send()
            for j in range(1, 4):
                for c in self.across(i, j):
                    c.wait_send()
            for j in range(4):
                for c in self.inside(i, j):
                    c.wait()
        for c in self.keep_own():
            c.wait()

    @staticmethod
    def scratch(rows_1, width):
        return [
            pltpu.VMEM((rows_1, width), BF), pltpu.SemaphoreType.DMA((2,)),
            pltpu.SemaphoreType.DMA((2 * Gather.SEMS,)), pltpu.SemaphoreType.DMA((2 * Gather.SEMS,)),
        ]


class Scatter:
    def __init__(self, term, own, came, sums, others, load_sems, pair_sems, z_sems):
        self.term, self.own, self.came, self.sums, self.others = term, own, came, sums, others
        self.load_sems, self.pair_sems, self.z_sems = load_sems, pair_sems, z_sems
        self.n = own.shape[1]

    @staticmethod
    def scratch(shape):
        n = shape[0] // 8
        blocks = lambda k: pltpu.VMEM((k, n, shape[1]), BF)
        return [blocks(Z), blocks(Z), blocks(Z), blocks(Z - 1), pltpu.SemaphoreType.DMA((Z,)), pltpu.SemaphoreType.DMA((2, Z)), pltpu.SemaphoreType.DMA((2, Z - 1))]

    SCRATCH = 7

    def block(self, z, core):
        return self.term.at[pl.ds(pl.multiple_of((2 * z + core) * self.n, self.n), self.n), :]

    def pair(self):
        _, _, core = place()
        return [remote(self.block(t, 1 - core), self.came.at[t], self.pair_sems.at[0, t], self.pair_sems.at[1, t], *sibling()) for t in range(Z)]

    def loads(self):
        _, _, core = place()
        return [pltpu.make_async_copy(self.block(t, core), self.own.at[t], self.load_sems.at[t]) for t in range(Z)]

    def along_z(self):
        rep, z, core = place()
        return [remote(self.sums.at[(z + i) % Z], self.others.at[i - 1], self.z_sems.at[0, i - 1], self.z_sems.at[1, i - 1], rep, (z + i) % Z, core) for i in (2, 1, 3)]

    def begin(self):
        meet(z_peers() + [sibling()])
        for c in self.pair() + self.loads():
            c.start()

    def add_pair(self):
        for c in self.pair() + self.loads():
            c.wait()
        for t in range(Z):
            self.sums[t] = (self.own[t].astype(F32) + self.came[t].astype(F32)).astype(BF)

    def send(self):
        for c in self.along_z():
            c.start()

    def end(self, out):
        _, z, _ = place()
        for c in self.along_z():
            c.wait()
        total = self.sums[z].astype(F32)
        for i in range(Z - 1):
            total += self.others[i].astype(F32)
        out[...] = total.astype(BF)

    def run(self, out):
        step, last = pl.program_id(0), pl.num_programs(0) - 1
        pl.when(step == 0)(self.begin)
        pl.when(step == 1)(self.add_pair)
        pl.when(step == 2)(self.send)
        pl.when(step == last)(functools.partial(self.end, out))


def gather_kernel(gate_ref, up_ref, down_ref, w1_ref, w2_ref, *scratch):
    g = Gather(gate_ref, up_ref, down_ref, w1_ref, w2_ref, scratch[0], scratch[1:])
    g.join()
    g.begin()
    for i in (1, 3, 2):
        g.hand_on(i)
    for i in (1, 3, 2):
        g.pass_in(i)
    g.end()


def forward_kernel(h_ref, w1_ref, w2_ref, gate_ref, up_ref, down_ref, o_ref, next_w1_ref, next_w2_ref, p_ref, *scratch):
    g = Gather(gate_ref, up_ref, down_ref, next_w1_ref, next_w2_ref, scratch[0], scratch[1:])
    step = pl.program_id(0)
    pl.when(step == 0)(g.join)
    pl.when(step == 0)(g.begin)
    for at, i in ((2, 1), (3, 3), (4, 2)):
        pl.when(step == at)(functools.partial(g.hand_on, i))
    for at, i in ((5, 1), (6, 3), (7, 2)):
        pl.when(step == at)(functools.partial(g.pass_in, i))
    ff = w2_ref.shape[0]
    wide = h_ref[...].astype(F32)
    a = (wide * scale_of(wide)).astype(BF)
    for s, w in chunks(ff):
        gu = dot(a, w1_ref[:, 2 * s : 2 * (s + w)])
        gate, up = gu[:, :w], gu[:, w:]
        p_ref[:, s : s + w] = (gate * sigmoid(gate) * up).astype(BF)
    o_ref[...] = h_ref[...] + dot(p_ref[...], w2_ref[...]).astype(BF)
    pl.when(step == pl.num_programs(0) - 1)(g.end)


def with_scatter(kernel, inputs, outputs):
    def both(*refs):
        ins, term, rest = refs[:inputs], refs[inputs], refs[inputs + 1 :]
        outs, block, rest = rest[:outputs], rest[outputs], rest[outputs + 1 :]
        own, scratch = rest[: len(rest) - Scatter.SCRATCH], rest[len(rest) - Scatter.SCRATCH :]
        job = Scatter(term, *scratch)
        step, last = pl.program_id(0), pl.num_programs(0) - 1
        pl.when(step == 0)(job.begin)
        pl.when(step == 1)(job.add_pair)
        pl.when(step == 2)(job.send)
        kernel(*ins, *outs, *own)
        pl.when(step == last)(lambda: job.end(block))

    return both


def hidden_kernel(h_ref, by_ref, w1_ref, w2_ref, dgu_ref, at_ref, dw2_ref, p_ref, acc_ref):
    ff = w2_ref.shape[0]
    step = pl.program_id(0)
    wide = h_ref[...].astype(F32)
    a = (wide * scale_of(wide)).astype(BF)
    at_ref[...] = a.T
    by = by_ref[...]
    for s, w in chunks(ff):
        gu = dot(a, w1_ref[:, 2 * s : 2 * (s + w)])
        dp = dot_nt(by, w2_ref[s : s + w, :]).astype(BF).astype(F32)
        gate, up = gu[:, :w], gu[:, w:]
        sg = sigmoid(gate)
        silu = gate * sg
        p_ref[:, s : s + w] = (silu * up).astype(BF)
        dgu_ref[:, 2 * s : 2 * s + w] = (dp * up * (sg + silu * (1 - sg))).astype(BF)
        dgu_ref[:, 2 * s + w : 2 * (s + w)] = (dp * silu).astype(BF)
    term = dot(by.T, p_ref[...])

    @pl.when(step == 0)
    def _():
        acc_ref[...] = term

    @pl.when(step > 0)
    def _():
        acc_ref[...] += term

    @pl.when(step == pl.num_programs(0) - 1)
    def _():
        dw2_ref[...] = acc_ref[...].astype(BF).T


def weights_kernel(at_ref, dgu_ref, dw1_ref):
    dw1_ref[...] = dot(at_ref[...], dgu_ref[...]).astype(BF)


def input_kernel(h_ref, by_ref, dgu_ref, w1_ref, o_ref):
    da = dot_nt(dgu_ref[...], w1_ref[...]).astype(BF).astype(F32)
    wide = h_ref[...].astype(F32)
    scale = scale_of(wide)
    inner = jnp.mean(da * wide, -1, keepdims=True)
    o_ref[...] = by_ref[...] + (scale * da - (scale * scale * scale * inner) * wide).astype(BF)


def params(number=None):
    more = {} if number is None else {"collective_id": number, "has_side_effects": True}
    return pltpu.CompilerParams(dimension_semantics=("arbitrary",), vmem_limit_bytes=VMEM_LIMIT, **more)


def cost(flops, nbytes):
    return pl.CostEstimate(flops=flops, bytes_accessed=nbytes, transcendentals=0)


def whole(shape):
    return pl.BlockSpec(shape, lambda i: (0,) * len(shape))


def rows(width):
    return pl.BlockSpec((TM, width), lambda i: (i, 0))


def of_layer(t, n):
    return pl.BlockSpec((1, *t.shape[1:]), lambda i: (n, 0, 0))


ANY = pl.BlockSpec(memory_space=pl.ANY)


def shapes(*all_of):
    return [jax.ShapeDtypeStruct(s, BF) for s in all_of]


def gather(blocks, n, number):
    (_, r1, ff), (_, r2, d) = blocks[0].shape, blocks[2].shape
    return pl.pallas_call(
        gather_kernel, grid=(1,), name="gather",
        in_specs=[of_layer(t, n) for t in blocks], out_specs=[ANY, ANY],
        out_shape=shapes((8 * r1, 2 * ff), (8 * r2, d)),
        scratch_shapes=Gather.scratch(r1, 2 * ff), compiler_params=params(number), cost_estimate=cost(10**9, 10**6),
    )(*blocks)


def forward(h, w1, w2, blocks, n, number):
    t, d = h.shape
    ff = w2.shape[0]
    return pl.pallas_call(
        forward_kernel, grid=(t // TM,), name="forward",
        in_specs=[rows(d), whole(w1.shape), whole(w2.shape), *(of_layer(b, n) for b in blocks)], out_specs=[rows(d), ANY, ANY],
        out_shape=shapes((t, d), w1.shape, w2.shape),
        scratch_shapes=[pltpu.VMEM((TM, ff), BF), *Gather.scratch(blocks[0].shape[1], 2 * ff)],
        compiler_params=params(number), cost_estimate=cost(6 * t * d * ff, 4 * t * d),
    )(h, w1, w2, *blocks)


def call(kernel, name, grid, in_specs, out_specs, out_shape, scratch, flops, args, term=None, number=None):
    if term is not None:
        kernel = with_scatter(kernel, len(in_specs), len(out_specs))
        block = (term.shape[0] // 8, term.shape[1])
        in_specs, out_specs, args = [*in_specs, ANY], [*out_specs, whole(block)], (*args, term)
        out_shape, scratch = [*out_shape, block], [*scratch, *Scatter.scratch(term.shape)]
    return pl.pallas_call(
        kernel, grid=grid, name=name, in_specs=in_specs, out_specs=out_specs, out_shape=shapes(*out_shape),
        scratch_shapes=scratch, compiler_params=params(number), cost_estimate=cost(flops, 10**7),
    )(*args)


def hidden(h, by, w1, w2, **more):
    t, d = h.shape
    ff = w2.shape[0]
    return call(
        hidden_kernel, "hidden", (t // TM,), [rows(d), rows(d), whole(w1.shape), whole(w2.shape)],
        [rows(2 * ff), pl.BlockSpec((d, TM), lambda i: (0, i)), whole((ff, d))], [(t, 2 * ff), (d, t), (ff, d)],
        [pltpu.VMEM((TM, ff), BF), pltpu.VMEM((d, ff), F32)], 8 * t * d * ff, (h, by, w1, w2), **more,
    )


def by_weights(at, dgu, **more):
    d, t = at.shape
    n = dgu.shape[1]
    return call(
        weights_kernel, "by_weights", (n // 256,), [whole((d, t)), pl.BlockSpec((t, 256), lambda i: (0, i))],
        [pl.BlockSpec((d, 256), lambda i: (0, i))], [(d, n)], [], 2 * t * d * n, (at, dgu), **more,
    )


def by_input(h, by, dgu, w1, **more):
    t, d = h.shape
    n = dgu.shape[1]
    return call(
        input_kernel, "by_input", (t // TM,), [rows(d), rows(d), rows(n), whole(w1.shape)],
        [rows(d)], [(t, d)], [], 2 * t * d * n, (h, by, dgu, w1), **more,
    )


def solution(mesh):
    def step(x, dy, w_gate, w_up, w_down):
        x, by = x[0], dy[0]
        blocks = (w_gate, w_up, w_down)
        w1, w2 = gather(blocks, 0, 0)
        h, v1, v2 = forward(x, w1, w2, blocks, 1, 1)
        dgu, at, t2 = hidden(h, by, v1, v2)
        t1, g2_1 = by_weights(at, dgu, term=t2, number=2)
        (by,) = by_input(h, by, lax.optimization_barrier((dgu, t1))[0], v1)
        dgu, at, t2, g1_1 = hidden(x, by, w1, w2, term=t1, number=3)
        t1, g2_0 = by_weights(at, dgu, term=t2, number=4)
        by, g1_0 = by_input(x, by, dgu, w1, term=t1, number=5)
        gates, ups = zip(parted(g1_0), parted(g1_1))
        return by[None], jnp.stack(gates), jnp.stack(ups), jnp.stack((g2_0, g2_1))

    spread, by_rows = P(("rep", "dp"), None, None), P(None, "dp", None)
    group = P("rep", "dp", None)
    return jax.shard_map(
        step, mesh=mesh, in_specs=(spread, spread, by_rows, by_rows, by_rows),
        out_specs=(spread, group, group, group), check_vma=False,
    )
```

```python
import functools

import jax
import jax.numpy as jnp
from jax import lax
from jax.experimental import pallas as pl
from jax.experimental.pallas import tpu as pltpu
from jax.sharding import PartitionSpec as P

EPS = 1e-6
BF, F32 = jnp.bfloat16, jnp.float32
TM = 512
CH = 256
VMEM_LIMIT = 60 * 2**20


def dot(a, b):
    return jnp.dot(a, b, preferred_element_type=F32)


def dot_nt(a, b):
    return lax.dot_general(a, b, (((1,), (1,)), ((), ())), preferred_element_type=F32)


def chunks(ff):
    return [(s, min(CH, ff - s)) for s in range(0, ff, CH)]


def scale_of(wide):
    return lax.rsqrt(jnp.mean(wide * wide, -1, keepdims=True) + EPS)


def sigmoid(t):
    return 0.5 * jnp.tanh(0.5 * t) + 0.5


MESH = pl.DeviceIdType.MESH
Z = 4


def place():
    dp = lax.axis_index("dp")
    return lax.axis_index("rep"), dp // 2, dp % 2


def remote(src, dst, send, recv, rep, z, core):
    return pltpu.make_async_remote_copy(src_ref=src, dst_ref=dst, send_sem=send, recv_sem=recv, device_id=(rep, 2 * z + core), device_id_type=MESH)


def meet(peers):
    barrier = pltpu.get_barrier_semaphore()
    for rep, z, core in peers:
        pl.semaphore_signal(barrier, inc=1, device_id=(rep, 2 * z + core), device_id_type=MESH)
    pl.semaphore_wait(barrier, len(peers))


def z_peers():
    rep, z, core = place()
    return [(rep, (z + i) % Z, core) for i in range(1, Z)]


def rep_peers():
    rep, z, core = place()
    return [((rep + i) % 4, z, core) for i in range(1, 4)]


def sibling():
    rep, z, core = place()
    return rep, z, 1 - core


class Gather:
    SEMS = 3 + 9 + 13

    def __init__(self, gate, up, down, w1, w2, shard, sems):
        self.gate, self.up, self.down, self.w1, self.w2, self.shard, self.sems = gate, up, down, w1, w2, shard, sems
        self.local_sems, self.send_sems, self.recv_sems = sems
        self.r1, self.r2 = gate.shape[1], down.shape[1]
        self.cols = w2.shape[1] // 4

    def block(self, z, core):
        s = 2 * z + core
        return (
            self.w1.at[pl.ds(pl.multiple_of(s * self.r1, self.r1), self.r1), :],
            self.w2.at[pl.ds(pl.multiple_of(s * self.r2, self.r2), self.r2), :],
        )

    def quarter(self, z, core, q):
        s, n = 2 * z + core, self.r1 // 4
        return (
            self.w1.at[pl.ds(pl.multiple_of(s * self.r1 + q * n, n), n), :],
            self.w2.at[pl.ds(pl.multiple_of(s * self.r2, self.r2), self.r2), pl.ds(pl.multiple_of(q * self.cols, self.cols), self.cols)],
        )

    def copies(self, number, srcs, dsts, to):
        return [remote(s, d, self.send_sems.at[2 * number + i], self.recv_sems.at[2 * number + i], *to) for i, (s, d) in enumerate(zip(srcs, dsts))]

    def along_z(self, i):
        rep, z, core = place()
        n = self.r1 // 4
        own = (self.shard.at[pl.ds(pl.multiple_of(rep * n, n), n), :], self.down.at[0, :, pl.ds(pl.multiple_of(rep * self.cols, self.cols), self.cols)])
        return self.copies(i - 1, own, self.quarter(z, core, rep), (rep, (z + i) % Z, core))

    def across(self, i, j):
        rep, z, core = place()
        part = self.quarter((z + Z - i) % Z, core, rep)
        return self.copies(3 + 3 * (i - 1) + j - 1, part, part, ((rep + j) % 4, z, core))

    def inside(self, i, j):
        rep, z, core = place()
        part = self.quarter((z + Z - i) % Z, core, (rep + 4 - j) % 4)
        return self.copies(13 + 4 * (i - 1) + j, part, part, sibling())

    def inside_own(self):
        _, z, core = place()
        return self.copies(12, (self.shard, self.down.at[0]), self.block(z, core), sibling())

    def keep_own(self):
        _, z, core = place()
        return [pltpu.make_async_copy(s, d, self.local_sems.at[i]) for i, (s, d) in enumerate(zip((self.shard, self.down.at[0]), self.block(z, core)))]

    def join(self):
        for s, w in chunks(self.gate.shape[2]):
            self.shard[:, 2 * s : 2 * s + w] = self.gate[0, :, s : s + w]
            self.shard[:, 2 * s + w : 2 * (s + w)] = self.up[0, :, s : s + w]

    def begin(self):
        meet(z_peers() + rep_peers() + [sibling()])
        for i in (2, 1, 3):
            for c in self.along_z(i):
                c.start()
        for c in self.inside_own() + self.keep_own():
            c.start()

    def hand_on(self, i):
        for c in self.along_z(i):
            c.wait_recv()
        for j in range(1, 4):
            for c in self.across(i, j):
                c.start()
        for c in self.inside(i, 0):
            c.start()

    def pass_in(self, i):
        for j in range(1, 4):
            for c in self.across(i, j):
                c.wait_recv()
            for c in self.inside(i, j):
                c.start()

    def end(self):
        for c in self.inside_own():
            c.wait()
        for i in range(1, Z):
            for c in self.along_z(i):
                c.wait_send()
            for j in range(1, 4):
                for c in self.across(i, j):
                    c.wait_send()
            for j in range(4):
                for c in self.inside(i, j):
                    c.wait()
        for c in self.keep_own():
            c.wait()

    @staticmethod
    def scratch(rows_1, width):
        return [
            pltpu.VMEM((rows_1, width), BF), pltpu.SemaphoreType.DMA((2,)),
            pltpu.SemaphoreType.DMA((2 * Gather.SEMS,)), pltpu.SemaphoreType.DMA((2 * Gather.SEMS,)),
        ]


class Scatter:
    def __init__(self, term, came, sums, others, relay, onward, pair_sems, z_sems):
        self.term, self.came, self.sums, self.others, self.relay, self.onward = term, came, sums, others, relay, onward
        self.pair_sems, self.z_sems = pair_sems, z_sems
        self.n = sums.shape[1]
        rep, z, core = place()
        self.rep, self.z, self.core = rep, z, core
        self.is_end = (z == 0) | (z == 3)
        self.near = 1 + z // 3
        self.outer, self.inner = 3 * (z // 2), 3 - z

    @staticmethod
    def scratch(rows_of, width):
        blocks = lambda k: pltpu.VMEM((k, rows_of, width), BF)
        return [blocks(Z), blocks(Z), blocks(2), blocks(2), blocks(2), pltpu.SemaphoreType.DMA((2, Z)), pltpu.SemaphoreType.DMA((2, 4))]

    SCRATCH = 7

    def block(self, z, core):
        return self.term.at[pl.ds(pl.multiple_of((2 * z + core) * self.n, self.n), self.n), :]

    def pair(self):
        return [remote(self.block(t, 1 - self.core), self.came.at[t], self.pair_sems.at[0, t], self.pair_sems.at[1, t], *sibling()) for t in range(Z)]

    def copy(self, src, number, z):
        slot = self.others.at[number] if number < 2 else self.relay.at[number - 2]
        return remote(src, slot, self.z_sems.at[0, number], self.z_sems.at[1, number], self.rep, z, self.core)

    def ends_copies(self):
        z, near = self.z, self.near
        return [self.copy(self.sums.at[t], number, near) for number, t in ((2, 3 - z), (3, 3 - near), (0, near))]

    def direct(self):
        return self.copy(self.sums.at[self.outer], 0, self.outer)

    def onwards(self, i):
        return self.copy(self.onward.at[i], 1, 3 - self.outer) if i == 0 else self.copy2()

    def copy2(self):
        return remote(self.onward.at[1], self.others.at[1], self.z_sems.at[0, 2], self.z_sems.at[1, 1], self.rep, self.inner, self.core)

    def begin(self):
        for c in self.pair():
            c.start()

    def add_pair(self):
        for c in self.pair():
            c.wait()
        for t in range(Z):
            self.sums[t] = (self.block(t, self.core)[...].astype(F32) + self.came[t].astype(F32)).astype(BF)

    def send(self):
        @pl.when(self.is_end)
        def _():
            for c in self.ends_copies():
                c.start()

        @pl.when(jnp.logical_not(self.is_end))
        def _():
            self.direct().start()

    def add_relay(self, i):
        @pl.when(jnp.logical_not(self.is_end))
        def _():
            self.copy(self.onward.at[i], 2 + i, self.near).wait_recv()
            to = 3 - self.outer if i == 0 else self.inner
            self.onward[i] = (self.sums[to].astype(F32) + self.relay[i].astype(F32)).astype(BF)

    def send_relay(self, i):
        @pl.when(jnp.logical_not(self.is_end))
        def _():
            self.onwards(i).start()

    def end(self):
        for i in range(2):
            self.copy(self.onward.at[i], i, self.near).wait_recv()

        @pl.when(self.is_end)
        def _():
            for c in self.ends_copies():
                c.wait_send()

        @pl.when(jnp.logical_not(self.is_end))
        def _():
            self.direct().wait_send()
            for i in range(2):
                self.onwards(i).wait_send()

        total = self.sums[self.z].astype(F32) + self.others[0].astype(F32) + self.others[1].astype(F32)
        return total.astype(BF)


def gather_kernel(gate_ref, up_ref, down_ref, w1_ref, w2_ref, *scratch):
    g = Gather(gate_ref, up_ref, down_ref, w1_ref, w2_ref, scratch[0], scratch[1:])
    g.join()
    g.begin()
    for i in (2, 1, 3):
        g.hand_on(i)
    for i in (2, 1, 3):
        g.pass_in(i)
    g.end()


def forward_kernel(h_ref, w1_ref, w2_ref, gate_ref, up_ref, down_ref, o_ref, next_w1_ref, next_w2_ref, p_ref, *scratch):
    g = Gather(gate_ref, up_ref, down_ref, next_w1_ref, next_w2_ref, scratch[0], scratch[1:])
    step = pl.program_id(0)
    pl.when(step == 0)(g.join)
    pl.when(step == 0)(g.begin)
    for at, i in ((2, 2), (3, 1), (4, 3)):
        pl.when(step == at)(functools.partial(g.hand_on, i))
    for at, i in ((5, 2), (7, 1)):
        pl.when(step == at)(functools.partial(g.pass_in, i))
    ff = w2_ref.shape[0]
    wide = h_ref[...].astype(F32)
    a = (wide * scale_of(wide)).astype(BF)
    for s, w in chunks(ff):
        gu = dot(a, w1_ref[:, 2 * s : 2 * (s + w)])
        gate, up = gu[:, :w], gu[:, w:]
        p_ref[:, s : s + w] = (gate * sigmoid(gate) * up).astype(BF)
    o_ref[...] = h_ref[...] + dot(p_ref[...], w2_ref[...]).astype(BF)
    pl.when(step == pl.num_programs(0) - 1)(lambda: (g.pass_in(3), g.end()) and None)


def backward_kernel(tiles, h_ref, by_ref, w1_ref, w2_ref, o_ref, dgate_ref, dup_ref, ddown_ref, dgu_ref, at_ref, p_ref, acc_ref, dw1_ref, dw2_ref, *scratch):
    ff = w2_ref.shape[0]
    parts = halves(ff)
    runs = [[c for c in chunks(ff) if lo <= c[0] < hi] for lo, hi in parts]
    s1, s2, s3, s4, count = marks(tiles, ff)
    step = pl.program_id(0)
    n = Scatter.SCRATCH
    first, second = (
        Scatter(dw1_ref.at[:, 2 * lo : 2 * hi], *scratch[n * k : n * (k + 1)]) for k, (lo, hi) in enumerate(parts)
    )
    down = Scatter(dw2_ref, *scratch[2 * n :])
    before = [
        (s2, first.begin), (s2 + 1, first.add_pair), (s2 + 4, lambda: first.add_relay(0)), (s2 + 6, lambda: first.add_relay(1)),
        (s3, down.begin), (s3 + 2, down.add_pair), (s4 + 1, lambda: down.add_relay(0)), (s4 + 3, lambda: down.add_relay(1)),
        (s4, second.begin), (s4 + 1, second.add_pair), (s4 + 6, lambda: second.add_relay(0)),
    ]
    after = [
        (s2 + 1, first.send), (s2 + 4, lambda: first.send_relay(0)), (s2 + 6, lambda: first.send_relay(1)),
        (s3 + 2, down.send), (s4 + 1, lambda: down.send_relay(0)), (s4 + 3, lambda: down.send_relay(1)),
        (s4 + 1, second.send), (s4 + 6, lambda: second.send_relay(0)),
    ]

    def first_end():
        put(first.end(), runs[0])

    def put(block, of):
        start = 2 * of[0][0]
        for s, w in of:
            at = 2 * s - start
            dgate_ref[:, s : s + w] = block[:, at : at + w]
            dup_ref[:, s : s + w] = block[:, at + w : at + 2 * w]

    before.append((s3 + 1, first_end))
    pl.when(step == 0)(lambda: meet(z_peers() + [sibling()]))
    for at, do in before:
        pl.when(step == at)(do)

    def hidden(part, tile):
        rows_of = pl.ds(pl.multiple_of(tile * TM, TM), TM)
        wide = h_ref[...].astype(F32)
        a = (wide * scale_of(wide)).astype(BF)
        if part == 0:
            at_ref[:, rows_of] = a.T
        by = by_ref[...]
        lo, hi = parts[part]
        for s, w in runs[part]:
            gu = dot(a, w1_ref[:, 2 * s : 2 * (s + w)])
            dp = dot_nt(by, w2_ref[s : s + w, :]).astype(BF).astype(F32)
            gate, up = gu[:, :w], gu[:, w:]
            sg = sigmoid(gate)
            silu = gate * sg
            p_ref[:, s - lo : s - lo + w] = (silu * up).astype(BF)
            dgu_ref[rows_of, 2 * s : 2 * s + w] = (dp * up * (sg + silu * (1 - sg))).astype(BF)
            dgu_ref[rows_of, 2 * s + w : 2 * (s + w)] = (dp * silu).astype(BF)
        term = dot(by.T, p_ref[:, : hi - lo])

        @pl.when(tile == 0)
        def _():
            acc_ref[:, lo:hi] = term

        @pl.when(tile > 0)
        def _():
            acc_ref[:, lo:hi] += term

        if part == 1:

            @pl.when(tile == tiles - 1)
            def _():
                dw2_ref[...] = acc_ref[...].astype(BF).T

    pl.when(step < s1)(lambda: hidden(0, step))
    pl.when((step >= s2) & (step < s3))(lambda: hidden(1, step - s2))

    def weights(number):
        columns = pl.ds(pl.multiple_of(number * 256, 256), 256)
        dw1_ref[:, columns] = dot(at_ref[...], dgu_ref[:, columns]).astype(BF)

    pl.when(((step >= s1) & (step < s2)) | ((step >= s3) & (step < s4)))(
        lambda: weights(jnp.where(step < s2, step - s1, step - s3 + s2 - s1))
    )

    @pl.when(step >= s4)
    def _():
        rows_of = pl.ds(pl.multiple_of((step - s4) * TM, TM), TM)
        da = dot_nt(dgu_ref[rows_of, :], w1_ref[...]).astype(BF).astype(F32)
        wide = h_ref[...].astype(F32)
        scale = scale_of(wide)
        inner = jnp.mean(da * wide, -1, keepdims=True)
        o_ref[...] = by_ref[...] + (scale * da - (scale * scale * scale * inner) * wide).astype(BF)

    for at, do in after:
        pl.when(step == at)(do)

    @pl.when(step == count - 1)
    def _():
        second.add_relay(1)
        ddown_ref[...] = down.end()
        second.send_relay(1)
        put(second.end(), runs[1])


def halves(ff):
    cut = chunks(ff)[(len(chunks(ff)) + 1) // 2][0]
    return (0, cut), (cut, ff)


def marks(tiles, ff):
    (_, cut), _ = halves(ff)
    a, b = 2 * cut // 256, 2 * (ff - cut) // 256
    return tiles, tiles + a, 2 * tiles + a, 2 * tiles + a + b, 3 * tiles + a + b


def params(number=None):
    more = {} if number is None else {"collective_id": number, "has_side_effects": True}
    return pltpu.CompilerParams(dimension_semantics=("arbitrary",), vmem_limit_bytes=VMEM_LIMIT, **more)


def cost(flops, nbytes):
    return pl.CostEstimate(flops=flops, bytes_accessed=nbytes, transcendentals=0)


def whole(shape):
    return pl.BlockSpec(shape, lambda i: (0,) * len(shape))


def rows(width):
    return pl.BlockSpec((TM, width), lambda i: (i, 0))


def of_layer(t, n):
    return pl.BlockSpec((1, *t.shape[1:]), lambda i: (n, 0, 0))


ANY = pl.BlockSpec(memory_space=pl.ANY)


def shapes(*all_of):
    return [jax.ShapeDtypeStruct(s, BF) for s in all_of]


def gather(blocks, n, number):
    (_, r1, ff), (_, r2, d) = blocks[0].shape, blocks[2].shape
    return pl.pallas_call(
        gather_kernel, grid=(1,), name="gather",
        in_specs=[of_layer(t, n) for t in blocks], out_specs=[ANY, ANY],
        out_shape=shapes((8 * r1, 2 * ff), (8 * r2, d)),
        scratch_shapes=Gather.scratch(r1, 2 * ff), compiler_params=params(number), cost_estimate=cost(10**9, 10**6),
    )(*blocks)


def forward(h, w1, w2, blocks, n, number):
    t, d = h.shape
    ff = w2.shape[0]
    return pl.pallas_call(
        forward_kernel, grid=(t // TM,), name="forward",
        in_specs=[rows(d), whole(w1.shape), whole(w2.shape), *(of_layer(b, n) for b in blocks)], out_specs=[rows(d), ANY, ANY],
        out_shape=shapes((t, d), w1.shape, w2.shape),
        scratch_shapes=[pltpu.VMEM((TM, ff), BF), *Gather.scratch(blocks[0].shape[1], 2 * ff)],
        compiler_params=params(number), cost_estimate=cost(6 * t * d * ff, 4 * t * d),
    )(h, w1, w2, *blocks)


def once(shape):
    return pl.BlockSpec(shape, lambda i: (0,) * len(shape), pipeline_mode=pl.Buffered(buffer_count=1))


def backward(h, by, w1, w2, number):
    t, d = h.shape
    ff = w2.shape[0]
    tiles = t // TM
    s1, s2, s3, s4, count = marks(tiles, ff)

    def tile(i):
        return jnp.where(i < s1, i, jnp.where(i < s2, 0, jnp.where(i < s3, i - s2, jnp.where(i < s4, 0, i - s4)))), 0

    r1, r2 = d // 8, ff // 8
    (_, cut), _ = halves(ff)
    return pl.pallas_call(
        functools.partial(backward_kernel, tiles), grid=(count,), name="backward",
        in_specs=[pl.BlockSpec((TM, d), tile), pl.BlockSpec((TM, d), tile), once(w1.shape), once(w2.shape)],
        out_specs=[pl.BlockSpec((TM, d), lambda i: (jnp.maximum(i - s4, 0), 0)), whole((r1, ff)), whole((r1, ff)), whole((r2, d))],
        out_shape=shapes((t, d), (r1, ff), (r1, ff), (r2, d)),
        scratch_shapes=[
            pltpu.VMEM((t, 2 * ff), BF), pltpu.VMEM((d, t), BF), pltpu.VMEM((TM, cut), BF), pltpu.VMEM((d, ff), F32),
            pltpu.VMEM((d, 2 * ff), BF), pltpu.VMEM((ff, d), BF),
            *Scatter.scratch(r1, 2 * cut), *Scatter.scratch(r1, 2 * (ff - cut)), *Scatter.scratch(r2, d),
        ],
        compiler_params=params(number), cost_estimate=cost(16 * t * d * ff, 10**7),
    )(h, by, w1, w2)


def solution(mesh):
    def step(x, dy, w_gate, w_up, w_down):
        x, by = x[0], dy[0]
        blocks = (w_gate, w_up, w_down)
        w1, w2 = gather(blocks, 0, 0)
        h, v1, v2 = forward(x, w1, w2, blocks, 1, 1)
        by, *last = backward(h, by, v1, v2, 2)
        by, *first = backward(x, by, w1, w2, 3)
        return (by[None], *(jnp.stack(pair) for pair in zip(first, last)))

    spread, by_rows = P(("rep", "dp"), None, None), P(None, "dp", None)
    group = P("rep", "dp", None)
    return jax.shard_map(
        step, mesh=mesh, in_specs=(spread, spread, by_rows, by_rows, by_rows),
        out_specs=(spread, group, group, group), check_vma=False,
    )
```

```python
import copy
import functools

import jax
import jax.numpy as jnp
from jax import lax
from jax.experimental import pallas as pl
from jax.experimental.pallas import tpu as pltpu
from jax.sharding import PartitionSpec as P

EPS = 1e-6
BF, F32 = jnp.bfloat16, jnp.float32
TM = 512
CH = 256
VMEM_LIMIT = 60 * 2**20


def dot(a, b):
    return jnp.dot(a, b, preferred_element_type=F32)


def dot_nt(a, b):
    return lax.dot_general(a, b, (((1,), (1,)), ((), ())), preferred_element_type=F32)


def chunks(ff):
    return [(s, min(CH, ff - s)) for s in range(0, ff, CH)]


def scale_of(wide):
    return lax.rsqrt(jnp.mean(wide * wide, -1, keepdims=True) + EPS)


def sigmoid(t):
    return 0.5 * jnp.tanh(0.5 * t) + 0.5


MESH = pl.DeviceIdType.MESH
Z = 4


def place():
    dp = lax.axis_index("dp")
    return lax.axis_index("rep"), dp // 2, dp % 2


def remote(src, dst, send, recv, rep, z, core):
    return pltpu.make_async_remote_copy(src_ref=src, dst_ref=dst, send_sem=send, recv_sem=recv, device_id=(rep, 2 * z + core), device_id_type=MESH)


def meet(peers):
    barrier = pltpu.get_barrier_semaphore()
    for rep, z, core in peers:
        pl.semaphore_signal(barrier, inc=1, device_id=(rep, 2 * z + core), device_id_type=MESH)
    pl.semaphore_wait(barrier, len(peers))


def z_peers():
    rep, z, core = place()
    return [(rep, (z + i) % Z, core) for i in range(1, Z)]


def rep_peers():
    rep, z, core = place()
    return [((rep + i) % 4, z, core) for i in range(1, 4)]


def sibling():
    rep, z, core = place()
    return rep, z, 1 - core


class Gather:
    SEMS = 3 + 9 + 13

    def __init__(self, gate, up, down, w1, w2, shard, sems):
        self.gate, self.up, self.down, self.w1, self.w2, self.shard, self.sems = gate, up, down, w1, w2, shard, sems
        self.local_sems, self.send_sems, self.recv_sems = sems
        self.r1, self.r2 = gate.shape[1], down.shape[1]
        self.cols = w2.shape[1] // 4
        self.which = (0, 1)

    def only(self, *which):
        part = copy.copy(self)
        part.which = which
        return part

    def block(self, z, core):
        s = 2 * z + core
        return (
            self.w1.at[pl.ds(pl.multiple_of(s * self.r1, self.r1), self.r1), :],
            self.w2.at[pl.ds(pl.multiple_of(s * self.r2, self.r2), self.r2), :],
        )

    def quarter(self, z, core, q):
        s, n = 2 * z + core, self.r1 // 4
        return (
            self.w1.at[pl.ds(pl.multiple_of(s * self.r1 + q * n, n), n), :],
            self.w2.at[pl.ds(pl.multiple_of(s * self.r2, self.r2), self.r2), pl.ds(pl.multiple_of(q * self.cols, self.cols), self.cols)],
        )

    def copies(self, number, srcs, dsts, to):
        return [remote(srcs[i], dsts[i], self.send_sems.at[2 * number + i], self.recv_sems.at[2 * number + i], *to) for i in self.which]

    def along_z(self, i):
        rep, z, core = place()
        n = self.r1 // 4
        own = (self.shard.at[pl.ds(pl.multiple_of(rep * n, n), n), :], self.down.at[0, :, pl.ds(pl.multiple_of(rep * self.cols, self.cols), self.cols)])
        return self.copies(i - 1, own, self.quarter(z, core, rep), (rep, (z + i) % Z, core))

    def across(self, i, j):
        rep, z, core = place()
        part = self.quarter((z + Z - i) % Z, core, rep)
        return self.copies(3 + 3 * (i - 1) + j - 1, part, part, ((rep + j) % 4, z, core))

    def inside(self, i, j):
        rep, z, core = place()
        part = self.quarter((z + Z - i) % Z, core, (rep + 4 - j) % 4)
        return self.copies(13 + 4 * (i - 1) + j, part, part, sibling())

    def inside_own(self):
        _, z, core = place()
        return self.copies(12, (self.shard, self.down.at[0]), self.block(z, core), sibling())

    def keep_own(self):
        _, z, core = place()
        srcs, dsts = (self.shard, self.down.at[0]), self.block(z, core)
        return [pltpu.make_async_copy(srcs[i], dsts[i], self.local_sems.at[i]) for i in self.which]

    def join(self):
        for s, w in chunks(self.gate.shape[2]):
            self.shard[:, 2 * s : 2 * s + w] = self.gate[0, :, s : s + w]
            self.shard[:, 2 * s + w : 2 * (s + w)] = self.up[0, :, s : s + w]

    def begin(self):
        for i in (2, 1, 3):
            for c in self.along_z(i):
                c.start()
        for c in self.inside_own() + self.keep_own():
            c.start()

    def hand_on(self, i):
        for c in self.along_z(i):
            c.wait_recv()
        for j in range(1, 4):
            for c in self.across(i, j):
                c.start()
        for c in self.inside(i, 0):
            c.start()

    def pass_in(self, i):
        for j in range(1, 4):
            for c in self.across(i, j):
                c.wait_recv()
            for c in self.inside(i, j):
                c.start()

    def arrived(self):
        for c in self.inside_own():
            c.wait_recv()
        for i in range(1, Z):
            for j in range(4):
                for c in self.inside(i, j):
                    c.wait_recv()
        for c in self.keep_own():
            c.wait()

    def sent(self):
        for c in self.inside_own():
            c.wait_send()
        for i in range(1, Z):
            for c in self.along_z(i):
                c.wait_send()
            for j in range(1, 4):
                for c in self.across(i, j):
                    c.wait_send()
            for j in range(4):
                for c in self.inside(i, j):
                    c.wait_send()

    @staticmethod
    def scratch(rows_1, width):
        return [
            pltpu.VMEM((rows_1, width), BF), pltpu.SemaphoreType.DMA((2,)),
            pltpu.SemaphoreType.DMA((2 * Gather.SEMS,)), pltpu.SemaphoreType.DMA((2 * Gather.SEMS,)),
        ]


class Scatter:
    def __init__(self, term, came, sums, others, relay, onward, pair_sems, z_sems):
        self.term, self.came, self.sums, self.others, self.relay, self.onward = term, came, sums, others, relay, onward
        self.pair_sems, self.z_sems = pair_sems, z_sems
        self.n = sums.shape[1]
        rep, z, core = place()
        self.rep, self.z, self.core = rep, z, core
        self.is_end = (z == 0) | (z == 3)
        self.near = 1 + z // 3
        self.outer, self.inner = 3 * (z // 2), 3 - z

    @staticmethod
    def scratch(rows_of, width):
        blocks = lambda k: pltpu.VMEM((k, rows_of, width), BF)
        return [blocks(Z), blocks(Z), blocks(2), blocks(2), blocks(2), pltpu.SemaphoreType.DMA((2, Z)), pltpu.SemaphoreType.DMA((2, 4))]

    SCRATCH = 7

    def block(self, z, core):
        return self.term.at[pl.ds(pl.multiple_of((2 * z + core) * self.n, self.n), self.n), :]

    def pair(self):
        return [remote(self.block(t, 1 - self.core), self.came.at[t], self.pair_sems.at[0, t], self.pair_sems.at[1, t], *sibling()) for t in range(Z)]

    def copy(self, src, number, z):
        slot = self.others.at[number] if number < 2 else self.relay.at[number - 2]
        return remote(src, slot, self.z_sems.at[0, number], self.z_sems.at[1, number], self.rep, z, self.core)

    def ends_copies(self):
        z, near = self.z, self.near
        return [self.copy(self.sums.at[t], number, near) for number, t in ((2, 3 - z), (3, 3 - near), (0, near))]

    def direct(self):
        return self.copy(self.sums.at[self.outer], 0, self.outer)

    def onwards(self, i):
        return self.copy(self.onward.at[i], 1, 3 - self.outer) if i == 0 else self.copy2()

    def copy2(self):
        return remote(self.onward.at[1], self.others.at[1], self.z_sems.at[0, 2], self.z_sems.at[1, 1], self.rep, self.inner, self.core)

    def begin(self):
        for c in self.pair():
            c.start()

    def add_pair(self):
        for c in self.pair():
            c.wait()
        for t in range(Z):
            self.sums[t] = (self.block(t, self.core)[...].astype(F32) + self.came[t].astype(F32)).astype(BF)

    def send(self):
        @pl.when(self.is_end)
        def _():
            for c in self.ends_copies():
                c.start()

        @pl.when(jnp.logical_not(self.is_end))
        def _():
            self.direct().start()

    def add_relay(self, i):
        @pl.when(jnp.logical_not(self.is_end))
        def _():
            self.copy(self.onward.at[i], 2 + i, self.near).wait_recv()
            to = 3 - self.outer if i == 0 else self.inner
            self.onward[i] = (self.sums[to].astype(F32) + self.relay[i].astype(F32)).astype(BF)

    def send_relay(self, i):
        @pl.when(jnp.logical_not(self.is_end))
        def _():
            self.onwards(i).start()

    def end(self):
        for i in range(2):
            self.copy(self.onward.at[i], i, self.near).wait_recv()

        @pl.when(self.is_end)
        def _():
            for c in self.ends_copies():
                c.wait_send()

        @pl.when(jnp.logical_not(self.is_end))
        def _():
            self.direct().wait_send()
            for i in range(2):
                self.onwards(i).wait_send()

        total = self.sums[self.z].astype(F32) + self.others[0].astype(F32) + self.others[1].astype(F32)
        return total.astype(BF)


ORDER = (2, 1, 3)


def forward_kernel(
    tiles, h_ref, gates, ups, downs, next_gates, next_ups, next_downs,
    o_ref, w1_ref, w2_ref, next_w1_ref, next_w2_ref, v1_ref, v2_ref, p_ref, out_sems, *scratch,
):
    half = len(scratch) // 2
    now = Gather(gates, ups, downs, v1_ref, v2_ref, scratch[0], scratch[1:half])
    later = Gather(next_gates, next_ups, next_downs, next_w1_ref, next_w2_ref, scratch[half], scratch[half + 1 :])
    step = pl.program_id(0)
    w1, w2 = now.only(0), now.only(1)
    next_w1, next_w2 = later.only(0), later.only(1)
    out = [pltpu.make_async_copy(v, w, out_sems.at[i]) for i, (v, w) in enumerate(((v1_ref, w1_ref), (v2_ref, w2_ref)))]

    @pl.when(step == 0)
    def _():
        now.join()
        meet(z_peers() + rep_peers() + [sibling()])
        w1.begin()
        w2.begin()
        later.join()
        for i in ORDER:
            w1.hand_on(i)
        next_w1.begin()
        for i in ORDER:
            w2.hand_on(i)
        for i in ORDER:
            w1.pass_in(i)
        next_w2.begin()
        w1.arrived()
        out[0].start()

    for at, do in (
        (1, lambda: [w2.pass_in(2), next_w1.hand_on(2)]), (2, lambda: [w2.pass_in(1), next_w1.hand_on(1)]),
        (3, lambda: [w2.pass_in(3), next_w1.hand_on(3)]), (4, lambda: next_w2.hand_on(2)), (5, lambda: next_w2.hand_on(1)),
        (6, lambda: next_w2.hand_on(3)), (8, lambda: [w2.arrived(), out[1].start()]), (9, lambda: next_w1.pass_in(2)),
        (10, lambda: next_w1.pass_in(1)), (11, lambda: next_w1.pass_in(3)), (13, lambda: next_w2.pass_in(2)), (14, lambda: next_w2.pass_in(1)),
    ):
        pl.when(step == at)(lambda do=do: do() and None)

    ff = v2_ref.shape[0]
    rows_of = pl.ds(pl.multiple_of(step % tiles * TM, TM), TM)

    @pl.when(step < tiles)
    def _():
        wide = h_ref[...].astype(F32)
        a = (wide * scale_of(wide)).astype(BF)
        for s, w in chunks(ff):
            gu = dot(a, v1_ref[:, 2 * s : 2 * (s + w)])
            gate, up = gu[:, :w], gu[:, w:]
            p_ref[rows_of, s : s + w] = (gate * sigmoid(gate) * up).astype(BF)

    @pl.when(step >= tiles)
    def _():
        o_ref[...] = h_ref[...] + dot(p_ref[rows_of, :], v2_ref[...]).astype(BF)

    @pl.when(step == 2 * tiles - 1)
    def _():
        next_w2.pass_in(3)
        later.arrived()
        now.sent()
        later.sent()
        for c in out:
            c.wait()


def backward_kernel(tiles, h_ref, by_ref, w1_ref, w2_ref, o_ref, dgate_ref, dup_ref, ddown_ref, dgu_ref, at_ref, p_ref, acc_ref, dw1_ref, dw2_ref, *scratch):
    ff = w2_ref.shape[0]
    parts = halves(ff)
    runs = [[c for c in chunks(ff) if lo <= c[0] < hi] for lo, hi in parts]
    s1, s2, s3, s4, count = marks(tiles, ff)
    step = pl.program_id(0)
    n = Scatter.SCRATCH
    first, second = (
        Scatter(dw1_ref.at[:, 2 * lo : 2 * hi], *scratch[n * k : n * (k + 1)]) for k, (lo, hi) in enumerate(parts)
    )
    down = Scatter(dw2_ref, *scratch[2 * n :])
    before = [
        (s2, first.begin), (s2 + 1, first.add_pair), (s2 + 4, lambda: first.add_relay(0)), (s2 + 6, lambda: first.add_relay(1)),
        (s3, down.begin), (s3 + 2, down.add_pair), (s4 + 1, lambda: down.add_relay(0)), (s4 + 3, lambda: down.add_relay(1)),
        (s4, second.begin), (s4 + 1, second.add_pair), (s4 + 6, lambda: second.add_relay(0)),
    ]
    after = [
        (s2 + 1, first.send), (s2 + 4, lambda: first.send_relay(0)), (s2 + 6, lambda: first.send_relay(1)),
        (s3 + 2, down.send), (s4 + 1, lambda: down.send_relay(0)), (s4 + 3, lambda: down.send_relay(1)),
        (s4 + 1, second.send), (s4 + 6, lambda: second.send_relay(0)),
    ]

    def first_end():
        put(first.end(), runs[0])

    def put(block, of):
        start = 2 * of[0][0]
        for s, w in of:
            at = 2 * s - start
            dgate_ref[:, s : s + w] = block[:, at : at + w]
            dup_ref[:, s : s + w] = block[:, at + w : at + 2 * w]

    before.append((s3 + 1, first_end))
    pl.when(step == 0)(lambda: meet(z_peers() + [sibling()]))
    for at, do in before:
        pl.when(step == at)(do)

    def hidden(part, tile):
        rows_of = pl.ds(pl.multiple_of(tile * TM, TM), TM)
        wide = h_ref[...].astype(F32)
        a = (wide * scale_of(wide)).astype(BF)
        if part == 0:
            at_ref[:, rows_of] = a.T
        by = by_ref[...]
        lo, hi = parts[part]
        for s, w in runs[part]:
            gu = dot(a, w1_ref[:, 2 * s : 2 * (s + w)])
            dp = dot_nt(by, w2_ref[s : s + w, :]).astype(BF).astype(F32)
            gate, up = gu[:, :w], gu[:, w:]
            sg = sigmoid(gate)
            silu = gate * sg
            p_ref[:, s - lo : s - lo + w] = (silu * up).astype(BF)
            dgu_ref[rows_of, 2 * s : 2 * s + w] = (dp * up * (sg + silu * (1 - sg))).astype(BF)
            dgu_ref[rows_of, 2 * s + w : 2 * (s + w)] = (dp * silu).astype(BF)
        term = dot(by.T, p_ref[:, : hi - lo])

        @pl.when(tile == 0)
        def _():
            acc_ref[:, lo:hi] = term

        @pl.when(tile > 0)
        def _():
            acc_ref[:, lo:hi] += term

        if part == 1:

            @pl.when(tile == tiles - 1)
            def _():
                dw2_ref[...] = acc_ref[...].astype(BF).T

    pl.when(step < s1)(lambda: hidden(0, step))
    pl.when((step >= s2) & (step < s3))(lambda: hidden(1, step - s2))

    def weights(number):
        columns = pl.ds(pl.multiple_of(number * 256, 256), 256)
        dw1_ref[:, columns] = dot(at_ref[...], dgu_ref[:, columns]).astype(BF)

    pl.when(((step >= s1) & (step < s2)) | ((step >= s3) & (step < s4)))(
        lambda: weights(jnp.where(step < s2, step - s1, step - s3 + s2 - s1))
    )

    @pl.when(step >= s4)
    def _():
        rows_of = pl.ds(pl.multiple_of((step - s4) * TM, TM), TM)
        da = dot_nt(dgu_ref[rows_of, :], w1_ref[...]).astype(BF).astype(F32)
        wide = h_ref[...].astype(F32)
        scale = scale_of(wide)
        inner = jnp.mean(da * wide, -1, keepdims=True)
        o_ref[...] = by_ref[...] + (scale * da - (scale * scale * scale * inner) * wide).astype(BF)

    for at, do in after:
        pl.when(step == at)(do)

    @pl.when(step == count - 1)
    def _():
        second.add_relay(1)
        ddown_ref[...] = down.end()
        second.send_relay(1)
        put(second.end(), runs[1])


def halves(ff):
    cut = chunks(ff)[(len(chunks(ff)) + 1) // 2][0]
    return (0, cut), (cut, ff)


def marks(tiles, ff):
    (_, cut), _ = halves(ff)
    a, b = 2 * cut // 256, 2 * (ff - cut) // 256
    return tiles, tiles + a, 2 * tiles + a, 2 * tiles + a + b, 3 * tiles + a + b


def params(number=None):
    more = {} if number is None else {"collective_id": number, "has_side_effects": True}
    return pltpu.CompilerParams(dimension_semantics=("arbitrary",), vmem_limit_bytes=VMEM_LIMIT, **more)


def cost(flops, nbytes):
    return pl.CostEstimate(flops=flops, bytes_accessed=nbytes, transcendentals=0)


def whole(shape):
    return pl.BlockSpec(shape, lambda i: (0,) * len(shape))


def rows(width):
    return pl.BlockSpec((TM, width), lambda i: (i, 0))


def of_layer(t, n):
    return pl.BlockSpec((1, *t.shape[1:]), lambda i: (n, 0, 0))


ANY = pl.BlockSpec(memory_space=pl.ANY)


def shapes(*all_of):
    return [jax.ShapeDtypeStruct(s, BF) for s in all_of]


def forward(h, blocks, number):
    t, d = h.shape
    (_, r1, ff), r2 = blocks[0].shape, blocks[2].shape[1]
    tiles = t // TM
    w1, w2 = (8 * r1, 2 * ff), (8 * r2, d)
    return pl.pallas_call(
        functools.partial(forward_kernel, tiles), grid=(2 * tiles,), name="forward",
        in_specs=[pl.BlockSpec((TM, d), lambda i: (i % tiles, 0)), *(of_layer(b, n) for n in range(2) for b in blocks)],
        out_specs=[pl.BlockSpec((TM, d), lambda i: (jnp.maximum(i - tiles, 0), 0)), ANY, ANY, ANY, ANY],
        out_shape=shapes((t, d), w1, w2, w1, w2),
        scratch_shapes=[
            pltpu.VMEM(w1, BF), pltpu.VMEM(w2, BF), pltpu.VMEM((t, ff), BF), pltpu.SemaphoreType.DMA((2,)),
            *Gather.scratch(r1, 2 * ff), *Gather.scratch(r1, 2 * ff),
        ],
        compiler_params=params(number), cost_estimate=cost(6 * t * d * ff, 4 * t * d),
    )(h, *blocks, *blocks)


def once(shape):
    return pl.BlockSpec(shape, lambda i: (0,) * len(shape), pipeline_mode=pl.Buffered(buffer_count=1))


def backward(h, by, w1, w2, number):
    t, d = h.shape
    ff = w2.shape[0]
    tiles = t // TM
    s1, s2, s3, s4, count = marks(tiles, ff)

    def tile(i):
        return jnp.where(i < s1, i, jnp.where(i < s2, 0, jnp.where(i < s3, i - s2, jnp.where(i < s4, 0, i - s4)))), 0

    r1, r2 = d // 8, ff // 8
    (_, cut), _ = halves(ff)
    return pl.pallas_call(
        functools.partial(backward_kernel, tiles), grid=(count,), name="backward",
        in_specs=[pl.BlockSpec((TM, d), tile), pl.BlockSpec((TM, d), tile), once(w1.shape), once(w2.shape)],
        out_specs=[pl.BlockSpec((TM, d), lambda i: (jnp.maximum(i - s4, 0), 0)), whole((r1, ff)), whole((r1, ff)), whole((r2, d))],
        out_shape=shapes((t, d), (r1, ff), (r1, ff), (r2, d)),
        scratch_shapes=[
            pltpu.VMEM((t, 2 * ff), BF), pltpu.VMEM((d, t), BF), pltpu.VMEM((TM, cut), BF), pltpu.VMEM((d, ff), F32),
            pltpu.VMEM((d, 2 * ff), BF), pltpu.VMEM((ff, d), BF),
            *Scatter.scratch(r1, 2 * cut), *Scatter.scratch(r1, 2 * (ff - cut)), *Scatter.scratch(r2, d),
        ],
        compiler_params=params(number), cost_estimate=cost(16 * t * d * ff, 10**7),
    )(h, by, w1, w2)


def solution(mesh):
    def step(x, dy, w_gate, w_up, w_down):
        x, by = x[0], dy[0]
        blocks = (w_gate, w_up, w_down)
        h, w1, w2, v1, v2 = forward(x, blocks, 1)
        by, *last = backward(h, by, v1, v2, 2)
        by, *first = backward(x, by, w1, w2, 3)
        return (by[None], *(jnp.stack(pair) for pair in zip(first, last)))

    spread, by_rows = P(("rep", "dp"), None, None), P(None, "dp", None)
    group = P("rep", "dp", None)
    return jax.shard_map(
        step, mesh=mesh, in_specs=(spread, spread, by_rows, by_rows, by_rows),
        out_specs=(spread, group, group, group), check_vma=False,
    )
```

```python
import copy
import functools

import jax
import jax.numpy as jnp
from jax import lax
from jax.experimental import pallas as pl
from jax.experimental.pallas import tpu as pltpu
from jax.sharding import PartitionSpec as P

EPS = 1e-6
BF, F32 = jnp.bfloat16, jnp.float32
TM = 512
TB = 1024
CH = 256
VMEM_LIMIT = 60 * 2**20


def dot(a, b):
    return jnp.dot(a, b, preferred_element_type=F32)


def dot_nt(a, b):
    return lax.dot_general(a, b, (((1,), (1,)), ((), ())), preferred_element_type=F32)


def chunks(ff):
    return [(s, min(CH, ff - s)) for s in range(0, ff, CH)]


def scale_of(wide):
    return lax.rsqrt(jnp.mean(wide * wide, -1, keepdims=True) + EPS)


def sigmoid(t):
    return 0.5 * jnp.tanh(0.5 * t) + 0.5


MESH = pl.DeviceIdType.MESH
Z = 4


def place():
    dp = lax.axis_index("dp")
    return lax.axis_index("rep"), dp // 2, dp % 2


def remote(src, dst, send, recv, rep, z, core):
    return pltpu.make_async_remote_copy(src_ref=src, dst_ref=dst, send_sem=send, recv_sem=recv, device_id=(rep, 2 * z + core), device_id_type=MESH)


def meet(peers):
    barrier = pltpu.get_barrier_semaphore()
    for rep, z, core in peers:
        pl.semaphore_signal(barrier, inc=1, device_id=(rep, 2 * z + core), device_id_type=MESH)
    pl.semaphore_wait(barrier, len(peers))


def z_peers():
    rep, z, core = place()
    return [(rep, (z + i) % Z, core) for i in range(1, Z)]


def rep_peers():
    rep, z, core = place()
    return [((rep + i) % 4, z, core) for i in range(1, 4)]


def sibling():
    rep, z, core = place()
    return rep, z, 1 - core


class Gather:
    SEMS = 3 + 9 + 13

    def __init__(self, gate, up, down, w1, w2, shard, sems):
        self.gate, self.up, self.down, self.w1, self.w2, self.shard, self.sems = gate, up, down, w1, w2, shard, sems
        self.local_sems, self.send_sems, self.recv_sems = sems
        self.r1, self.r2 = gate.shape[1], down.shape[1]
        self.cols = w2.shape[1] // 4
        self.which = (0, 1)

    def only(self, *which):
        part = copy.copy(self)
        part.which = which
        return part

    def block(self, z, core):
        s = 2 * z + core
        return (
            self.w1.at[pl.ds(pl.multiple_of(s * self.r1, self.r1), self.r1), :],
            self.w2.at[pl.ds(pl.multiple_of(s * self.r2, self.r2), self.r2), :],
        )

    def quarter(self, z, core, q):
        s, n = 2 * z + core, self.r1 // 4
        return (
            self.w1.at[pl.ds(pl.multiple_of(s * self.r1 + q * n, n), n), :],
            self.w2.at[pl.ds(pl.multiple_of(s * self.r2, self.r2), self.r2), pl.ds(pl.multiple_of(q * self.cols, self.cols), self.cols)],
        )

    def copies(self, number, srcs, dsts, to):
        return [remote(srcs[i], dsts[i], self.send_sems.at[2 * number + i], self.recv_sems.at[2 * number + i], *to) for i in self.which]

    def along_z(self, i):
        rep, z, core = place()
        n = self.r1 // 4
        own = (self.shard.at[pl.ds(pl.multiple_of(rep * n, n), n), :], self.down.at[0, :, pl.ds(pl.multiple_of(rep * self.cols, self.cols), self.cols)])
        return self.copies(i - 1, own, self.quarter(z, core, rep), (rep, (z + i) % Z, core))

    def across(self, i, j):
        rep, z, core = place()
        part = self.quarter((z + Z - i) % Z, core, rep)
        return self.copies(3 + 3 * (i - 1) + j - 1, part, part, ((rep + j) % 4, z, core))

    def inside(self, i, j):
        rep, z, core = place()
        part = self.quarter((z + Z - i) % Z, core, (rep + 4 - j) % 4)
        return self.copies(13 + 4 * (i - 1) + j, part, part, sibling())

    def inside_own(self):
        _, z, core = place()
        return self.copies(12, (self.shard, self.down.at[0]), self.block(z, core), sibling())

    def keep_own(self):
        _, z, core = place()
        srcs, dsts = (self.shard, self.down.at[0]), self.block(z, core)
        return [pltpu.make_async_copy(srcs[i], dsts[i], self.local_sems.at[i]) for i in self.which]

    def join(self):
        for s, w in chunks(self.gate.shape[2]):
            self.shard[:, 2 * s : 2 * s + w] = self.gate[0, :, s : s + w]
            self.shard[:, 2 * s + w : 2 * (s + w)] = self.up[0, :, s : s + w]

    def begin(self):
        for i in (2, 1, 3):
            for c in self.along_z(i):
                c.start()
        for c in self.inside_own() + self.keep_own():
            c.start()

    def hand_on(self, i):
        for c in self.along_z(i):
            c.wait_recv()
        for j in range(1, 4):
            for c in self.across(i, j):
                c.start()
        for c in self.inside(i, 0):
            c.start()

    def pass_in(self, i):
        for j in range(1, 4):
            for c in self.across(i, j):
                c.wait_recv()
            for c in self.inside(i, j):
                c.start()

    def arrived(self):
        for c in self.inside_own():
            c.wait_recv()
        for i in range(1, Z):
            for j in range(4):
                for c in self.inside(i, j):
                    c.wait_recv()
        for c in self.keep_own():
            c.wait()

    def sent(self):
        for c in self.inside_own():
            c.wait_send()
        for i in range(1, Z):
            for c in self.along_z(i):
                c.wait_send()
            for j in range(1, 4):
                for c in self.across(i, j):
                    c.wait_send()
            for j in range(4):
                for c in self.inside(i, j):
                    c.wait_send()

    @staticmethod
    def scratch(rows_1, width):
        return [
            pltpu.VMEM((rows_1, width), BF), pltpu.SemaphoreType.DMA((2,)),
            pltpu.SemaphoreType.DMA((2 * Gather.SEMS,)), pltpu.SemaphoreType.DMA((2 * Gather.SEMS,)),
        ]


class Scatter:
    def __init__(self, term, came, sums, others, relay, onward, pair_sems, z_sems):
        self.term, self.came, self.sums, self.others, self.relay, self.onward = term, came, sums, others, relay, onward
        self.pair_sems, self.z_sems = pair_sems, z_sems
        self.n = sums.shape[1]
        rep, z, core = place()
        self.rep, self.z, self.core = rep, z, core
        self.is_end = (z == 0) | (z == 3)
        self.near = 1 + z // 3
        self.outer, self.inner = 3 * (z // 2), 3 - z

    @staticmethod
    def scratch(rows_of, width):
        blocks = lambda k: pltpu.VMEM((k, rows_of, width), BF)
        return [blocks(Z), blocks(Z), blocks(2), blocks(2), blocks(2), pltpu.SemaphoreType.DMA((2, Z)), pltpu.SemaphoreType.DMA((2, 4))]

    SCRATCH = 7

    def block(self, z, core):
        return self.term.at[pl.ds(pl.multiple_of((2 * z + core) * self.n, self.n), self.n), :]

    def pair(self):
        return [remote(self.block(t, 1 - self.core), self.came.at[t], self.pair_sems.at[0, t], self.pair_sems.at[1, t], *sibling()) for t in range(Z)]

    def copy(self, src, number, z):
        slot = self.others.at[number] if number < 2 else self.relay.at[number - 2]
        return remote(src, slot, self.z_sems.at[0, number], self.z_sems.at[1, number], self.rep, z, self.core)

    def ends_copies(self):
        z, near = self.z, self.near
        return [self.copy(self.sums.at[t], number, near) for number, t in ((2, 3 - z), (3, 3 - near), (0, near))]

    def direct(self):
        return self.copy(self.sums.at[self.outer], 0, self.outer)

    def onwards(self, i):
        return self.copy(self.onward.at[i], 1, 3 - self.outer) if i == 0 else self.copy2()

    def copy2(self):
        return remote(self.onward.at[1], self.others.at[1], self.z_sems.at[0, 2], self.z_sems.at[1, 1], self.rep, self.inner, self.core)

    def begin(self):
        for c in self.pair():
            c.start()

    def add_pair(self):
        for c in self.pair():
            c.wait()
        for t in range(Z):
            self.sums[t] = (self.block(t, self.core)[...].astype(F32) + self.came[t].astype(F32)).astype(BF)

    def send(self):
        @pl.when(self.is_end)
        def _():
            for c in self.ends_copies():
                c.start()

        @pl.when(jnp.logical_not(self.is_end))
        def _():
            self.direct().start()

    def add_relay(self, i):
        @pl.when(jnp.logical_not(self.is_end))
        def _():
            self.copy(self.onward.at[i], 2 + i, self.near).wait_recv()
            to = 3 - self.outer if i == 0 else self.inner
            self.onward[i] = (self.sums[to].astype(F32) + self.relay[i].astype(F32)).astype(BF)

    def send_relay(self, i):
        @pl.when(jnp.logical_not(self.is_end))
        def _():
            self.onwards(i).start()

    def end(self):
        for i in range(2):
            self.copy(self.onward.at[i], i, self.near).wait_recv()

        @pl.when(self.is_end)
        def _():
            for c in self.ends_copies():
                c.wait_send()

        @pl.when(jnp.logical_not(self.is_end))
        def _():
            self.direct().wait_send()
            for i in range(2):
                self.onwards(i).wait_send()

        total = self.sums[self.z].astype(F32) + self.others[0].astype(F32) + self.others[1].astype(F32)
        return total.astype(BF)


ORDER = (2, 1, 3)


def forward_kernel(
    tiles, h_ref, gates, ups, downs, next_gates, next_ups, next_downs,
    o_ref, w1_ref, w2_ref, next_w1_ref, next_w2_ref, v1_ref, v2_ref, p_ref, out_sems, *scratch,
):
    half = len(scratch) // 2
    now = Gather(gates, ups, downs, v1_ref, v2_ref, scratch[0], scratch[1:half])
    later = Gather(next_gates, next_ups, next_downs, next_w1_ref, next_w2_ref, scratch[half], scratch[half + 1 :])
    step = pl.program_id(0)
    w1, w2 = now.only(0), now.only(1)
    next_w1, next_w2 = later.only(0), later.only(1)
    out = [pltpu.make_async_copy(v, w, out_sems.at[i]) for i, (v, w) in enumerate(((v1_ref, w1_ref), (v2_ref, w2_ref)))]

    @pl.when(step == 0)
    def _():
        now.join()
        meet(z_peers() + rep_peers() + [sibling()])
        w1.begin()
        w2.begin()
        later.join()
        for i in ORDER:
            w1.hand_on(i)
        next_w1.begin()
        for i in ORDER:
            w2.hand_on(i)
        for i in ORDER:
            w1.pass_in(i)
        next_w2.begin()
        w1.arrived()
        out[0].start()

    for at, do in (
        (1, lambda: [w2.pass_in(2), next_w1.hand_on(2)]), (2, lambda: [w2.pass_in(1), next_w1.hand_on(1)]),
        (3, lambda: [w2.pass_in(3), next_w1.hand_on(3)]), (4, lambda: next_w2.hand_on(2)), (5, lambda: next_w2.hand_on(1)),
        (6, lambda: next_w2.hand_on(3)), (8, lambda: [w2.arrived(), out[1].start()]), (9, lambda: next_w1.pass_in(2)),
        (10, lambda: next_w1.pass_in(1)), (11, lambda: next_w1.pass_in(3)), (13, lambda: next_w2.pass_in(2)), (14, lambda: next_w2.pass_in(1)),
    ):
        pl.when(step == at)(lambda do=do: do() and None)

    ff = v2_ref.shape[0]
    rows_of = pl.ds(pl.multiple_of(step % tiles * TM, TM), TM)

    @pl.when(step < tiles)
    def _():
        wide = h_ref[...].astype(F32)
        a = (wide * scale_of(wide)).astype(BF)
        for s, w in chunks(ff):
            gu = dot(a, v1_ref[:, 2 * s : 2 * (s + w)])
            gate, up = gu[:, :w], gu[:, w:]
            p_ref[rows_of, s : s + w] = (gate * sigmoid(gate) * up).astype(BF)

    @pl.when(step >= tiles)
    def _():
        o_ref[...] = h_ref[...] + dot(p_ref[rows_of, :], v2_ref[...]).astype(BF)

    @pl.when(step == 2 * tiles - 1)
    def _():
        next_w2.pass_in(3)
        later.arrived()
        now.sent()
        later.sent()
        for c in out:
            c.wait()


def backward_kernel(tiles, h_ref, by_ref, w1_ref, w2_ref, o_ref, dgate_ref, dup_ref, ddown_ref, dgu_ref, at_ref, p_ref, acc_ref, dw1_ref, dw2_ref, *scratch):
    ff = w2_ref.shape[0]
    parts = halves(ff)
    runs = [[c for c in chunks(ff) if lo <= c[0] < hi] for lo, hi in parts]
    s1, s2, s3, s4, count = marks(tiles, ff)
    step = pl.program_id(0)
    n = Scatter.SCRATCH
    first, second = (
        Scatter(dw1_ref.at[:, 2 * lo : 2 * hi], *scratch[n * k : n * (k + 1)]) for k, (lo, hi) in enumerate(parts)
    )
    down = Scatter(dw2_ref, *scratch[2 * n :])
    before = [
        (s2, first.begin), (s2 + 1, first.send), (s2 + 3, lambda: first.send_relay(0)), (s3, lambda: first.send_relay(1)),
        (s3, down.begin), (s3 + 1, down.send), (s4, lambda: down.send_relay(0)), (s4 + 1, lambda: down.send_relay(1)),
        (s4, second.begin), (s4 + 1, second.send), (s4 + 3, lambda: second.send_relay(0)),
    ]
    after = [
        (s2, first.add_pair), (s2 + 2, lambda: first.add_relay(0)), (s2 + 3, lambda: first.add_relay(1)),
        (s3, down.add_pair), (s4 - 1, lambda: down.add_relay(0)), (s4, lambda: down.add_relay(1)),
        (s4, second.add_pair), (s4 + 2, lambda: second.add_relay(0)),
    ]

    def first_end():
        put(first.end(), runs[0])

    def put(block, of):
        start = 2 * of[0][0]
        for s, w in of:
            at = 2 * s - start
            dgate_ref[:, s : s + w] = block[:, at : at + w]
            dup_ref[:, s : s + w] = block[:, at + w : at + 2 * w]

    before.append((s4, first_end))
    pl.when(step == 0)(lambda: meet(z_peers() + [sibling()]))
    for at, do in before:
        pl.when(step == at)(do)

    def hidden(part, tile):
        rows_of = pl.ds(pl.multiple_of(tile * TB, TB), TB)
        wide = h_ref[...].astype(F32)
        a = (wide * scale_of(wide)).astype(BF)
        if part == 0:
            at_ref[:, rows_of] = a.T
        by = by_ref[...]
        lo, hi = parts[part]
        for s, w in runs[part]:
            gu = dot(a, w1_ref[:, 2 * s : 2 * (s + w)])
            dp = dot_nt(by, w2_ref[s : s + w, :]).astype(BF).astype(F32)
            gate, up = gu[:, :w], gu[:, w:]
            sg = sigmoid(gate)
            silu = gate * sg
            p_ref[:, s - lo : s - lo + w] = (silu * up).astype(BF)
            dgu_ref[rows_of, 2 * s : 2 * s + w] = (dp * up * (sg + silu * (1 - sg))).astype(BF)
            dgu_ref[rows_of, 2 * s + w : 2 * (s + w)] = (dp * silu).astype(BF)
        term = dot(by.T, p_ref[:, : hi - lo])

        @pl.when(tile == 0)
        def _():
            acc_ref[:, lo:hi] = term

        @pl.when(tile > 0)
        def _():
            acc_ref[:, lo:hi] += term

        if part == 1:

            @pl.when(tile == tiles - 1)
            def _():
                dw2_ref[...] = acc_ref[...].astype(BF).T

    pl.when(step < s1)(lambda: hidden(0, step))
    pl.when((step >= s2) & (step < s3))(lambda: hidden(1, step - s2))

    def weights(number):
        columns = pl.ds(pl.multiple_of(number * 256, 256), 256)
        dw1_ref[:, columns] = dot(at_ref[...], dgu_ref[:, columns]).astype(BF)

    pl.when(((step >= s1) & (step < s2)) | ((step >= s3) & (step < s4)))(
        lambda: weights(jnp.where(step < s2, step - s1, step - s3 + s2 - s1))
    )

    @pl.when(step >= s4)
    def _():
        rows_of = pl.ds(pl.multiple_of((step - s4) * TB, TB), TB)
        da = dot_nt(dgu_ref[rows_of, :], w1_ref[...]).astype(BF).astype(F32)
        wide = h_ref[...].astype(F32)
        scale = scale_of(wide)
        inner = jnp.mean(da * wide, -1, keepdims=True)
        o_ref[...] = by_ref[...] + (scale * da - (scale * scale * scale * inner) * wide).astype(BF)

    for at, do in after:
        pl.when(step == at)(do)

    @pl.when(step == count - 1)
    def _():
        second.add_relay(1)
        ddown_ref[...] = down.end()
        second.send_relay(1)
        put(second.end(), runs[1])


def halves(ff):
    cut = chunks(ff)[(len(chunks(ff)) + 1) // 2][0]
    return (0, cut), (cut, ff)


def marks(tiles, ff):
    (_, cut), _ = halves(ff)
    a, b = 2 * cut // 256, 2 * (ff - cut) // 256
    return tiles, tiles + a, 2 * tiles + a, 2 * tiles + a + b, 3 * tiles + a + b


def params(number=None):
    more = {} if number is None else {"collective_id": number, "has_side_effects": True}
    return pltpu.CompilerParams(dimension_semantics=("arbitrary",), vmem_limit_bytes=VMEM_LIMIT, **more)


def cost(flops, nbytes):
    return pl.CostEstimate(flops=flops, bytes_accessed=nbytes, transcendentals=0)


def whole(shape):
    return pl.BlockSpec(shape, lambda i: (0,) * len(shape))


def rows(width):
    return pl.BlockSpec((TM, width), lambda i: (i, 0))


def of_layer(t, n):
    return pl.BlockSpec((1, *t.shape[1:]), lambda i: (n, 0, 0))


ANY = pl.BlockSpec(memory_space=pl.ANY)


def shapes(*all_of):
    return [jax.ShapeDtypeStruct(s, BF) for s in all_of]


def forward(h, blocks, number):
    t, d = h.shape
    (_, r1, ff), r2 = blocks[0].shape, blocks[2].shape[1]
    tiles = t // TM
    w1, w2 = (8 * r1, 2 * ff), (8 * r2, d)
    return pl.pallas_call(
        functools.partial(forward_kernel, tiles), grid=(2 * tiles,), name="forward",
        in_specs=[pl.BlockSpec((TM, d), lambda i: (i % tiles, 0)), *(of_layer(b, n) for n in range(2) for b in blocks)],
        out_specs=[pl.BlockSpec((TM, d), lambda i: (jnp.maximum(i - tiles, 0), 0)), ANY, ANY, ANY, ANY],
        out_shape=shapes((t, d), w1, w2, w1, w2),
        scratch_shapes=[
            pltpu.VMEM(w1, BF), pltpu.VMEM(w2, BF), pltpu.VMEM((t, ff), BF), pltpu.SemaphoreType.DMA((2,)),
            *Gather.scratch(r1, 2 * ff), *Gather.scratch(r1, 2 * ff),
        ],
        compiler_params=params(number), cost_estimate=cost(6 * t * d * ff, 4 * t * d),
    )(h, *blocks, *blocks)


def once(shape):
    return pl.BlockSpec(shape, lambda i: (0,) * len(shape), pipeline_mode=pl.Buffered(buffer_count=1))


def backward(h, by, w1, w2, number):
    t, d = h.shape
    ff = w2.shape[0]
    tiles = t // TB
    s1, s2, s3, s4, count = marks(tiles, ff)

    def tile(i):
        return jnp.where(i < s1, i, jnp.where(i < s2, 0, jnp.where(i < s3, i - s2, jnp.where(i < s4, 0, i - s4)))), 0

    r1, r2 = d // 8, ff // 8
    (_, cut), _ = halves(ff)
    return pl.pallas_call(
        functools.partial(backward_kernel, tiles), grid=(count,), name="backward",
        in_specs=[pl.BlockSpec((TB, d), tile), pl.BlockSpec((TB, d), tile), once(w1.shape), once(w2.shape)],
        out_specs=[pl.BlockSpec((TB, d), lambda i: (jnp.maximum(i - s4, 0), 0)), whole((r1, ff)), whole((r1, ff)), whole((r2, d))],
        out_shape=shapes((t, d), (r1, ff), (r1, ff), (r2, d)),
        scratch_shapes=[
            pltpu.VMEM((t, 2 * ff), BF), pltpu.VMEM((d, t), BF), pltpu.VMEM((TB, cut), BF), pltpu.VMEM((d, ff), F32),
            pltpu.VMEM((d, 2 * ff), BF), pltpu.VMEM((ff, d), BF),
            *Scatter.scratch(r1, 2 * cut), *Scatter.scratch(r1, 2 * (ff - cut)), *Scatter.scratch(r2, d),
        ],
        compiler_params=params(number), cost_estimate=cost(16 * t * d * ff, 10**7),
    )(h, by, w1, w2)


def solution(mesh):
    def step(x, dy, w_gate, w_up, w_down):
        x, by = x[0], dy[0]
        blocks = (w_gate, w_up, w_down)
        h, w1, w2, v1, v2 = forward(x, blocks, 1)
        by, *last = backward(h, by, v1, v2, 2)
        by, *first = backward(x, by, w1, w2, 3)
        return (by[None], *(jnp.stack(pair) for pair in zip(first, last)))

    spread, by_rows = P(("rep", "dp"), None, None), P(None, "dp", None)
    group = P("rep", "dp", None)
    return jax.shard_map(
        step, mesh=mesh, in_specs=(spread, spread, by_rows, by_rows, by_rows),
        out_specs=(spread, group, group, group), check_vma=False,
    )
```

```python
import copy
import functools

import jax
import jax.numpy as jnp
from jax import lax
from jax.experimental import pallas as pl
from jax.experimental.pallas import tpu as pltpu
from jax.sharding import PartitionSpec as P

EPS = 1e-6
BF, F32 = jnp.bfloat16, jnp.float32
TM = 1024
CH = 256
VMEM_LIMIT = 60 * 2**20


def dot(a, b):
    return jnp.dot(a, b, preferred_element_type=F32)


def dot_nt(a, b):
    return lax.dot_general(a, b, (((1,), (1,)), ((), ())), preferred_element_type=F32)


def chunks(ff):
    return [(s, min(CH, ff - s)) for s in range(0, ff, CH)]


def scale_of(wide):
    return lax.rsqrt(jnp.mean(wide * wide, -1, keepdims=True) + EPS)


def sigmoid(t):
    return 0.5 * jnp.tanh(0.5 * t) + 0.5


MESH = pl.DeviceIdType.MESH
Z = 4


def place():
    dp = lax.axis_index("dp")
    return lax.axis_index("rep"), dp // 2, dp % 2


def remote(src, dst, send, recv, rep, z, core):
    return pltpu.make_async_remote_copy(src_ref=src, dst_ref=dst, send_sem=send, recv_sem=recv, device_id=(rep, 2 * z + core), device_id_type=MESH)


def meet(peers):
    barrier = pltpu.get_barrier_semaphore()
    for rep, z, core in peers:
        pl.semaphore_signal(barrier, inc=1, device_id=(rep, 2 * z + core), device_id_type=MESH)
    pl.semaphore_wait(barrier, len(peers))


def z_peers():
    rep, z, core = place()
    return [(rep, (z + i) % Z, core) for i in range(1, Z)]


def rep_peers():
    rep, z, core = place()
    return [((rep + i) % 4, z, core) for i in range(1, 4)]


def sibling():
    rep, z, core = place()
    return rep, z, 1 - core


class Gather:
    SEMS = 3 + 9 + 13

    def __init__(self, gate, up, down, w1, w2, shard, sems):
        self.gate, self.up, self.down, self.w1, self.w2, self.shard, self.sems = gate, up, down, w1, w2, shard, sems
        self.local_sems, self.send_sems, self.recv_sems = sems
        self.r1, self.r2 = gate.shape[1], down.shape[1]
        self.cols = w2.shape[1] // 4
        self.which = (0, 1)

    def only(self, *which):
        part = copy.copy(self)
        part.which = which
        return part

    def block(self, z, core):
        s = 2 * z + core
        return (
            self.w1.at[pl.ds(pl.multiple_of(s * self.r1, self.r1), self.r1), :],
            self.w2.at[pl.ds(pl.multiple_of(s * self.r2, self.r2), self.r2), :],
        )

    def quarter(self, z, core, q):
        s, n = 2 * z + core, self.r1 // 4
        return (
            self.w1.at[pl.ds(pl.multiple_of(s * self.r1 + q * n, n), n), :],
            self.w2.at[pl.ds(pl.multiple_of(s * self.r2, self.r2), self.r2), pl.ds(pl.multiple_of(q * self.cols, self.cols), self.cols)],
        )

    def copies(self, number, srcs, dsts, to):
        return [remote(srcs[i], dsts[i], self.send_sems.at[2 * number + i], self.recv_sems.at[2 * number + i], *to) for i in self.which]

    def along_z(self, i):
        rep, z, core = place()
        n = self.r1 // 4
        own = (self.shard.at[pl.ds(pl.multiple_of(rep * n, n), n), :], self.down.at[0, :, pl.ds(pl.multiple_of(rep * self.cols, self.cols), self.cols)])
        return self.copies(i - 1, own, self.quarter(z, core, rep), (rep, (z + i) % Z, core))

    def across(self, i, j):
        rep, z, core = place()
        part = self.quarter((z + Z - i) % Z, core, rep)
        return self.copies(3 + 3 * (i - 1) + j - 1, part, part, ((rep + j) % 4, z, core))

    def inside(self, i, j):
        rep, z, core = place()
        part = self.quarter((z + Z - i) % Z, core, (rep + 4 - j) % 4)
        return self.copies(13 + 4 * (i - 1) + j, part, part, sibling())

    def inside_own(self):
        _, z, core = place()
        return self.copies(12, (self.shard, self.down.at[0]), self.block(z, core), sibling())

    def keep_own(self):
        _, z, core = place()
        srcs, dsts = (self.shard, self.down.at[0]), self.block(z, core)
        return [pltpu.make_async_copy(srcs[i], dsts[i], self.local_sems.at[i]) for i in self.which]

    def join(self):
        for s, w in chunks(self.gate.shape[2]):
            self.shard[:, 2 * s : 2 * s + w] = self.gate[0, :, s : s + w]
            self.shard[:, 2 * s + w : 2 * (s + w)] = self.up[0, :, s : s + w]

    def begin(self):
        for i in (2, 1, 3):
            for c in self.along_z(i):
                c.start()
        for c in self.inside_own() + self.keep_own():
            c.start()

    def hand_on(self, i):
        for c in self.along_z(i):
            c.wait_recv()
        for j in range(1, 4):
            for c in self.across(i, j):
                c.start()
        for c in self.inside(i, 0):
            c.start()

    def pass_in(self, i):
        for j in range(1, 4):
            for c in self.across(i, j):
                c.wait_recv()
            for c in self.inside(i, j):
                c.start()

    def arrived(self):
        for c in self.inside_own():
            c.wait_recv()
        for i in range(1, Z):
            for j in range(4):
                for c in self.inside(i, j):
                    c.wait_recv()
        for c in self.keep_own():
            c.wait()

    def sent(self):
        for c in self.inside_own():
            c.wait_send()
        for i in range(1, Z):
            for c in self.along_z(i):
                c.wait_send()
            for j in range(1, 4):
                for c in self.across(i, j):
                    c.wait_send()
            for j in range(4):
                for c in self.inside(i, j):
                    c.wait_send()

    @staticmethod
    def scratch(rows_1, width):
        return [
            pltpu.VMEM((rows_1, width), BF), pltpu.SemaphoreType.DMA((2,)),
            pltpu.SemaphoreType.DMA((2 * Gather.SEMS,)), pltpu.SemaphoreType.DMA((2 * Gather.SEMS,)),
        ]


class Scatter:
    def __init__(self, term, came, sums, others, relay, onward, pair_sems, z_sems):
        self.term, self.came, self.sums, self.others, self.relay, self.onward = term, came, sums, others, relay, onward
        self.pair_sems, self.z_sems = pair_sems, z_sems
        self.n = sums.shape[1]
        rep, z, core = place()
        self.rep, self.z, self.core = rep, z, core
        self.is_end = (z == 0) | (z == 3)
        self.near = 1 + z // 3
        self.outer, self.inner = 3 * (z // 2), 3 - z

    @staticmethod
    def scratch(rows_of, width):
        blocks = lambda k: pltpu.VMEM((k, rows_of, width), BF)
        return [blocks(Z), blocks(Z), blocks(2), blocks(2), blocks(2), pltpu.SemaphoreType.DMA((2, Z)), pltpu.SemaphoreType.DMA((2, 4))]

    SCRATCH = 7

    def block(self, z, core):
        return self.term.at[pl.ds(pl.multiple_of((2 * z + core) * self.n, self.n), self.n), :]

    def pair(self):
        return [remote(self.block(t, 1 - self.core), self.came.at[t], self.pair_sems.at[0, t], self.pair_sems.at[1, t], *sibling()) for t in range(Z)]

    def copy(self, src, number, z):
        slot = self.others.at[number] if number < 2 else self.relay.at[number - 2]
        return remote(src, slot, self.z_sems.at[0, number], self.z_sems.at[1, number], self.rep, z, self.core)

    def ends_copies(self):
        z, near = self.z, self.near
        return [self.copy(self.sums.at[t], number, near) for number, t in ((2, 3 - z), (3, 3 - near), (0, near))]

    def direct(self):
        return self.copy(self.sums.at[self.outer], 0, self.outer)

    def onwards(self, i):
        return self.copy(self.onward.at[i], 1, 3 - self.outer) if i == 0 else self.copy2()

    def copy2(self):
        return remote(self.onward.at[1], self.others.at[1], self.z_sems.at[0, 2], self.z_sems.at[1, 1], self.rep, self.inner, self.core)

    def begin(self):
        for c in self.pair():
            c.start()

    def add_pair(self):
        for c in self.pair():
            c.wait()
        for t in range(Z):
            self.sums[t] = (self.block(t, self.core)[...].astype(F32) + self.came[t].astype(F32)).astype(BF)

    def send(self):
        @pl.when(self.is_end)
        def _():
            for c in self.ends_copies():
                c.start()

        @pl.when(jnp.logical_not(self.is_end))
        def _():
            self.direct().start()

    def add_relay(self, i):
        @pl.when(jnp.logical_not(self.is_end))
        def _():
            self.copy(self.onward.at[i], 2 + i, self.near).wait_recv()
            to = 3 - self.outer if i == 0 else self.inner
            self.onward[i] = (self.sums[to].astype(F32) + self.relay[i].astype(F32)).astype(BF)

    def send_relay(self, i):
        @pl.when(jnp.logical_not(self.is_end))
        def _():
            self.onwards(i).start()

    def end(self):
        for i in range(2):
            self.copy(self.onward.at[i], i, self.near).wait_recv()

        @pl.when(self.is_end)
        def _():
            for c in self.ends_copies():
                c.wait_send()

        @pl.when(jnp.logical_not(self.is_end))
        def _():
            self.direct().wait_send()
            for i in range(2):
                self.onwards(i).wait_send()

        total = self.sums[self.z].astype(F32) + self.others[0].astype(F32) + self.others[1].astype(F32)
        return total.astype(BF)


ORDER = (2, 1, 3)


def forward_kernel(
    tiles, h_ref, gates, ups, downs, next_gates, next_ups, next_downs,
    o_ref, w1_ref, w2_ref, next_w1_ref, next_w2_ref, v1_ref, v2_ref, p_ref, out_sems, *scratch,
):
    half = len(scratch) // 2
    now = Gather(gates, ups, downs, v1_ref, v2_ref, scratch[0], scratch[1:half])
    later = Gather(next_gates, next_ups, next_downs, next_w1_ref, next_w2_ref, scratch[half], scratch[half + 1 :])
    step = pl.program_id(0)
    w1, w2 = now.only(0), now.only(1)
    next_w1, next_w2 = later.only(0), later.only(1)
    out = [pltpu.make_async_copy(v, w, out_sems.at[i]) for i, (v, w) in enumerate(((v1_ref, w1_ref), (v2_ref, w2_ref)))]

    @pl.when(step == 0)
    def _():
        now.join()
        meet(z_peers() + rep_peers() + [sibling()])
        w1.begin()
        w2.begin()
        later.join()
        for i in ORDER:
            w1.hand_on(i)
        next_w1.begin()
        for i in ORDER:
            w2.hand_on(i)
        for i in ORDER:
            w1.pass_in(i)
        next_w2.begin()
        w1.arrived()
        out[0].start()

    def each(do):
        for i in ORDER:
            do(i)

    for at, do in (
        (1, lambda: [each(w2.pass_in), each(next_w1.hand_on)]), (2, lambda: each(next_w2.hand_on)),
        (tiles, lambda: [w2.arrived(), out[1].start()]), (tiles + 2, lambda: each(next_w1.pass_in)),
    ):
        pl.when(step == at)(lambda do=do: do() and None)

    ff = v2_ref.shape[0]
    rows_of = pl.ds(pl.multiple_of(step % tiles * TM, TM), TM)

    @pl.when(step < tiles)
    def _():
        wide = h_ref[...].astype(F32)
        a = (wide * scale_of(wide)).astype(BF)
        for s, w in chunks(ff):
            gu = dot(a, v1_ref[:, 2 * s : 2 * (s + w)])
            gate, up = gu[:, :w], gu[:, w:]
            p_ref[rows_of, s : s + w] = (gate * sigmoid(gate) * up).astype(BF)

    @pl.when(step >= tiles)
    def _():
        o_ref[...] = h_ref[...] + dot(p_ref[rows_of, :], v2_ref[...]).astype(BF)

    @pl.when(step == 2 * tiles - 1)
    def _():
        each(next_w2.pass_in)
        later.arrived()
        now.sent()
        later.sent()
        for c in out:
            c.wait()


def backward_kernel(tiles, kept, h_ref, by_ref, w1_ref, w2_ref, *refs):
    others, (o_ref, *grads, dgu_ref, at_ref, p_ref, acc_ref, dw1_ref, dw2_ref), scratch = refs[:kept], refs[kept : kept + 10], refs[kept + 10 :]
    dgate_ref, dup_ref, ddown_ref = (g.at[0] for g in grads)
    ff = w2_ref.shape[0]
    parts = halves(ff)
    runs = [[c for c in chunks(ff) if lo <= c[0] < hi] for lo, hi in parts]
    s1, s2, s3, s4, count = marks(tiles, ff)
    step = pl.program_id(0)
    n = Scatter.SCRATCH
    first, second = (
        Scatter(dw1_ref.at[:, 2 * lo : 2 * hi], *scratch[n * k : n * (k + 1)]) for k, (lo, hi) in enumerate(parts)
    )
    down = Scatter(dw2_ref, *scratch[2 * n :])
    before = [
        (s2, first.begin), (s2 + 1, first.send), (s2 + 3, lambda: first.send_relay(0)), (s3, lambda: first.send_relay(1)),
        (s3, down.begin), (s3 + 1, down.send), (s4, lambda: down.send_relay(0)), (s4 + 1, lambda: down.send_relay(1)),
        (s4, second.begin), (s4 + 1, second.send), (s4 + 3, lambda: second.send_relay(0)),
    ]
    after = [
        (s2, first.add_pair), (s2 + 2, lambda: first.add_relay(0)), (s2 + 3, lambda: first.add_relay(1)),
        (s3, down.add_pair), (s4 - 1, lambda: down.add_relay(0)), (s4, lambda: down.add_relay(1)),
        (s4, second.add_pair), (s4 + 2, lambda: second.add_relay(0)),
    ]

    def first_end():
        put(first.end(), runs[0])

    def put(block, of):
        start = 2 * of[0][0]
        for s, w in of:
            at = 2 * s - start
            dgate_ref[:, s : s + w] = block[:, at : at + w]
            dup_ref[:, s : s + w] = block[:, at + w : at + 2 * w]

    before.append((s4, first_end))
    pl.when(step == 0)(lambda: meet(z_peers() + [sibling()]))

    @pl.when(step == 1)
    def _():
        for other, grad in zip(others, grads):
            grad[1:] = other[...]

    for at, do in before:
        pl.when(step == at)(do)

    def hidden(part, tile):
        rows_of = pl.ds(pl.multiple_of(tile * TM, TM), TM)
        wide = h_ref[...].astype(F32)
        a = (wide * scale_of(wide)).astype(BF)
        if part == 0:
            at_ref[:, rows_of] = a.T
        by = by_ref[...]
        lo, hi = parts[part]
        for s, w in runs[part]:
            gu = dot(a, w1_ref[:, 2 * s : 2 * (s + w)])
            dp = dot_nt(by, w2_ref[s : s + w, :]).astype(BF).astype(F32)
            gate, up = gu[:, :w], gu[:, w:]
            sg = sigmoid(gate)
            silu = gate * sg
            p_ref[:, s - lo : s - lo + w] = (silu * up).astype(BF)
            dgu_ref[rows_of, 2 * s : 2 * s + w] = (dp * up * (sg + silu * (1 - sg))).astype(BF)
            dgu_ref[rows_of, 2 * s + w : 2 * (s + w)] = (dp * silu).astype(BF)
        term = dot(by.T, p_ref[:, : hi - lo])

        @pl.when(tile == 0)
        def _():
            acc_ref[:, lo:hi] = term

        @pl.when(tile > 0)
        def _():
            acc_ref[:, lo:hi] += term

        if part == 1:

            @pl.when(tile == tiles - 1)
            def _():
                dw2_ref[...] = acc_ref[...].astype(BF).T

    pl.when(step < s1)(lambda: hidden(0, step))
    pl.when((step >= s2) & (step < s3))(lambda: hidden(1, step - s2))

    def weights(number):
        columns = pl.ds(pl.multiple_of(number * 256, 256), 256)
        dw1_ref[:, columns] = dot(at_ref[...], dgu_ref[:, columns]).astype(BF)

    pl.when(((step >= s1) & (step < s2)) | ((step >= s3) & (step < s4)))(
        lambda: weights(jnp.where(step < s2, step - s1, step - s3 + s2 - s1))
    )

    @pl.when(step >= s4)
    def _():
        rows_of = pl.ds(pl.multiple_of((step - s4) * TM, TM), TM)
        da = dot_nt(dgu_ref[rows_of, :], w1_ref[...]).astype(BF).astype(F32)
        wide = h_ref[...].astype(F32)
        scale = scale_of(wide)
        inner = jnp.mean(da * wide, -1, keepdims=True)
        o_ref[...] = by_ref[...] + (scale * da - (scale * scale * scale * inner) * wide).astype(BF)

    for at, do in after:
        pl.when(step == at)(do)

    @pl.when(step == count - 1)
    def _():
        second.add_relay(1)
        ddown_ref[...] = down.end()
        second.send_relay(1)
        put(second.end(), runs[1])


def halves(ff):
    cut = chunks(ff)[(len(chunks(ff)) + 1) // 2][0]
    return (0, cut), (cut, ff)


def marks(tiles, ff):
    (_, cut), _ = halves(ff)
    a, b = 2 * cut // 256, 2 * (ff - cut) // 256
    return tiles, tiles + a, 2 * tiles + a, 2 * tiles + a + b, 3 * tiles + a + b


def params(number=None):
    more = {} if number is None else {"collective_id": number, "has_side_effects": True}
    return pltpu.CompilerParams(dimension_semantics=("arbitrary",), vmem_limit_bytes=VMEM_LIMIT, **more)


def cost(flops, nbytes):
    return pl.CostEstimate(flops=flops, bytes_accessed=nbytes, transcendentals=0)


def whole(shape):
    return pl.BlockSpec(shape, lambda i: (0,) * len(shape))


def rows(width):
    return pl.BlockSpec((TM, width), lambda i: (i, 0))


def of_layer(t, n):
    return pl.BlockSpec((1, *t.shape[1:]), lambda i: (n, 0, 0))


ANY = pl.BlockSpec(memory_space=pl.ANY)


def shapes(*all_of):
    return [jax.ShapeDtypeStruct(s, BF) for s in all_of]


def forward(h, blocks, number):
    t, d = h.shape
    (_, r1, ff), r2 = blocks[0].shape, blocks[2].shape[1]
    tiles = t // TM
    w1, w2 = (8 * r1, 2 * ff), (8 * r2, d)
    return pl.pallas_call(
        functools.partial(forward_kernel, tiles), grid=(2 * tiles,), name="forward",
        in_specs=[pl.BlockSpec((TM, d), lambda i: (i % tiles, 0)), *(of_layer(b, n) for n in range(2) for b in blocks)],
        out_specs=[pl.BlockSpec((TM, d), lambda i: (jnp.maximum(i - tiles, 0), 0)), ANY, ANY, ANY, ANY],
        out_shape=shapes((t, d), w1, w2, w1, w2),
        scratch_shapes=[
            pltpu.VMEM(w1, BF), pltpu.VMEM(w2, BF), pltpu.VMEM((t, ff), BF), pltpu.SemaphoreType.DMA((2,)),
            *Gather.scratch(r1, 2 * ff), *Gather.scratch(r1, 2 * ff),
        ],
        compiler_params=params(number), cost_estimate=cost(6 * t * d * ff, 4 * t * d),
    )(h, *blocks, *blocks)


def once(shape):
    return pl.BlockSpec(shape, lambda i: (0,) * len(shape), pipeline_mode=pl.Buffered(buffer_count=1))


def backward(h, by, w1, w2, number, others=()):
    t, d = h.shape
    ff = w2.shape[0]
    tiles = t // TM
    s1, s2, s3, s4, count = marks(tiles, ff)

    def tile(i):
        return jnp.where(i < s1, i, jnp.where(i < s2, 0, jnp.where(i < s3, i - s2, jnp.where(i < s4, 0, i - s4)))), 0

    r1, r2 = d // 8, ff // 8
    (_, cut), _ = halves(ff)
    count_of = 1 + sum(t.shape[0] for t in others[:1])
    blocks = [(count_of, r1, ff), (count_of, r1, ff), (count_of, r2, d)]
    return pl.pallas_call(
        functools.partial(backward_kernel, tiles, len(others)), grid=(count,), name="backward",
        in_specs=[pl.BlockSpec((TM, d), tile), pl.BlockSpec((TM, d), tile), once(w1.shape), once(w2.shape), *(once(t.shape) for t in others)],
        out_specs=[pl.BlockSpec((TM, d), lambda i: (jnp.maximum(i - s4, 0), 0)), *(once(b) for b in blocks)],
        out_shape=shapes((t, d), *blocks),
        scratch_shapes=[
            pltpu.VMEM((t, 2 * ff), BF), pltpu.VMEM((d, t), BF), pltpu.VMEM((TM, cut), BF), pltpu.VMEM((d, ff), F32),
            pltpu.VMEM((d, 2 * ff), BF), pltpu.VMEM((ff, d), BF),
            *Scatter.scratch(r1, 2 * cut), *Scatter.scratch(r1, 2 * (ff - cut)), *Scatter.scratch(r2, d),
        ],
        compiler_params=params(number), cost_estimate=cost(16 * t * d * ff, 10**7),
    )(h, by, w1, w2, *others)


def solution(mesh):
    def step(x, dy, w_gate, w_up, w_down):
        x, by = x[0], dy[0]
        blocks = (w_gate, w_up, w_down)
        h, w1, w2, v1, v2 = forward(x, blocks, 1)
        by, *last = backward(h, by, v1, v2, 2)
        by, *both = backward(x, by, w1, w2, 3, last)
        return (by[None], *both)

    spread, by_rows = P(("rep", "dp"), None, None), P(None, "dp", None)
    group = P("rep", "dp", None)
    return jax.shard_map(
        step, mesh=mesh, in_specs=(spread, spread, by_rows, by_rows, by_rows),
        out_specs=(spread, group, group, group), check_vma=False,
    )
```

```python
import copy
import functools

import jax
import jax.numpy as jnp
from jax import lax
from jax.experimental import pallas as pl
from jax.experimental.pallas import tpu as pltpu
from jax.sharding import PartitionSpec as P

EPS = 1e-6
BF, F32 = jnp.bfloat16, jnp.float32
TM = 1024
CH = 256
VMEM_LIMIT = 60 * 2**20


def dot(a, b):
    return jnp.dot(a, b, preferred_element_type=F32)


def dot_nt(a, b):
    return lax.dot_general(a, b, (((1,), (1,)), ((), ())), preferred_element_type=F32)


def chunks(ff):
    return [(s, min(CH, ff - s)) for s in range(0, ff, CH)]


def scale_of(wide):
    return lax.rsqrt(jnp.mean(wide * wide, -1, keepdims=True) + EPS)


def sigmoid(t):
    return 0.5 * jnp.tanh(0.5 * t) + 0.5


MESH = pl.DeviceIdType.MESH
Z = 4


def place():
    dp = lax.axis_index("dp")
    return lax.axis_index("rep"), dp // 2, dp % 2


def remote(src, dst, send, recv, rep, z, core):
    return pltpu.make_async_remote_copy(src_ref=src, dst_ref=dst, send_sem=send, recv_sem=recv, device_id=(rep, 2 * z + core), device_id_type=MESH)


def meet(peers):
    barrier = pltpu.get_barrier_semaphore()
    for rep, z, core in peers:
        pl.semaphore_signal(barrier, inc=1, device_id=(rep, 2 * z + core), device_id_type=MESH)
    pl.semaphore_wait(barrier, len(peers))


def z_peers():
    rep, z, core = place()
    return [(rep, (z + i) % Z, core) for i in range(1, Z)]


def rep_peers():
    rep, z, core = place()
    return [((rep + i) % 4, z, core) for i in range(1, 4)]


def sibling():
    rep, z, core = place()
    return rep, z, 1 - core


class Gather:
    SEMS = 3 + 9 + 13

    def __init__(self, gate, up, down, w1, w2, shard, sems):
        self.gate, self.up, self.down, self.w1, self.w2, self.shard, self.sems = gate, up, down, w1, w2, shard, sems
        self.local_sems, self.send_sems, self.recv_sems = sems
        self.r1, self.r2 = gate.shape[1], down.shape[1]
        self.cols = w2.shape[1] // 4
        self.which = (0, 1)

    def only(self, *which):
        part = copy.copy(self)
        part.which = which
        return part

    def block(self, z, core):
        s = 2 * z + core
        return (
            self.w1.at[pl.ds(pl.multiple_of(s * self.r1, self.r1), self.r1), :],
            self.w2.at[pl.ds(pl.multiple_of(s * self.r2, self.r2), self.r2), :],
        )

    def quarter(self, z, core, q):
        s, n = 2 * z + core, self.r1 // 4
        return (
            self.w1.at[pl.ds(pl.multiple_of(s * self.r1 + q * n, n), n), :],
            self.w2.at[pl.ds(pl.multiple_of(s * self.r2, self.r2), self.r2), pl.ds(pl.multiple_of(q * self.cols, self.cols), self.cols)],
        )

    def copies(self, number, srcs, dsts, to):
        return [remote(srcs[i], dsts[i], self.send_sems.at[2 * number + i], self.recv_sems.at[2 * number + i], *to) for i in self.which]

    def along_z(self, i):
        rep, z, core = place()
        n = self.r1 // 4
        own = (self.shard.at[pl.ds(pl.multiple_of(rep * n, n), n), :], self.down.at[0, :, pl.ds(pl.multiple_of(rep * self.cols, self.cols), self.cols)])
        return self.copies(i - 1, own, self.quarter(z, core, rep), (rep, (z + i) % Z, core))

    def diagonal(self, i):
        rep, z, core = place()
        odd, q = rep % 2, 3 - rep
        src = self.down.at[0, :, pl.ds(pl.multiple_of(q * self.cols, self.cols), self.cols)]
        number = 3 + 3 * (i - 1) - 1
        sems = self.send_sems.at[2 * (number + 3 - 2 * odd) + 1], self.recv_sems.at[2 * (number + 1 + 2 * odd) + 1]
        return remote(src, self.quarter(z, core, q)[1], *sems, rep, (z + i) % Z, core)

    def across(self, i, j):
        rep, z, core = place()
        part = self.quarter((z + Z - i) % Z, core, rep)
        return self.copies(3 + 3 * (i - 1) + j - 1, part, part, ((rep + j) % 4, z, core))

    def inside(self, i, j):
        rep, z, core = place()
        part = self.quarter((z + Z - i) % Z, core, (rep + 4 - j) % 4)
        return self.copies(13 + 4 * (i - 1) + j, part, part, sibling())

    def inside_own(self):
        _, z, core = place()
        return self.copies(12, (self.shard, self.down.at[0]), self.block(z, core), sibling())

    def keep_own(self):
        _, z, core = place()
        srcs, dsts = (self.shard, self.down.at[0]), self.block(z, core)
        return [pltpu.make_async_copy(srcs[i], dsts[i], self.local_sems.at[i]) for i in self.which]

    def join(self):
        for s, w in chunks(self.gate.shape[2]):
            self.shard[:, 2 * s : 2 * s + w] = self.gate[0, :, s : s + w]
            self.shard[:, 2 * s + w : 2 * (s + w)] = self.up[0, :, s : s + w]

    def begin(self):
        for i in (2, 1, 3):
            for c in self.along_z(i):
                c.start()
        if 1 in self.which:
            for i in (2, 1, 3):
                self.diagonal(i).start()
        for c in self.inside_own() + self.keep_own():
            c.start()

    def hand_on(self, i):
        for c in self.along_z(i):
            c.wait_recv()
        rep, _, _ = place()
        for j in range(1, 4):
            for which, c in zip(self.which, self.across(i, j)):
                if which == 0 or j == 2:
                    c.start()
                else:
                    pl.when(j != 3 - 2 * (rep % 2))(c.start)
        for c in self.inside(i, 0):
            c.start()

    def pass_in(self, i):
        for j in range(1, 4):
            for c in self.across(i, j):
                c.wait_recv()
            for c in self.inside(i, j):
                c.start()

    def arrived(self):
        for c in self.inside_own():
            c.wait_recv()
        for i in range(1, Z):
            for j in range(4):
                for c in self.inside(i, j):
                    c.wait_recv()
        for c in self.keep_own():
            c.wait()

    def sent(self):
        for c in self.inside_own():
            c.wait_send()
        for i in range(1, Z):
            for c in self.along_z(i):
                c.wait_send()
            for j in range(1, 4):
                for c in self.across(i, j):
                    c.wait_send()
            for j in range(4):
                for c in self.inside(i, j):
                    c.wait_send()

    @staticmethod
    def scratch(rows_1, width):
        return [
            pltpu.VMEM((rows_1, width), BF), pltpu.SemaphoreType.DMA((2,)),
            pltpu.SemaphoreType.DMA((2 * Gather.SEMS,)), pltpu.SemaphoreType.DMA((2 * Gather.SEMS,)),
        ]


class Scatter:
    def __init__(self, term, came, sums, others, relay, onward, pair_sems, z_sems):
        self.term, self.came, self.sums, self.others, self.relay, self.onward = term, came, sums, others, relay, onward
        self.pair_sems, self.z_sems = pair_sems, z_sems
        self.n = sums.shape[1]
        rep, z, core = place()
        self.rep, self.z, self.core = rep, z, core
        self.is_end = (z == 0) | (z == 3)
        self.near = 1 + z // 3
        self.outer, self.inner = 3 * (z // 2), 3 - z

    @staticmethod
    def scratch(rows_of, width):
        blocks = lambda k: pltpu.VMEM((k, rows_of, width), BF)
        return [blocks(Z), blocks(Z), blocks(2), blocks(2), blocks(2), pltpu.SemaphoreType.DMA((2, Z)), pltpu.SemaphoreType.DMA((2, 4))]

    SCRATCH = 7

    def block(self, z, core):
        return self.term.at[pl.ds(pl.multiple_of((2 * z + core) * self.n, self.n), self.n), :]

    def pair(self):
        return [remote(self.block(t, 1 - self.core), self.came.at[t], self.pair_sems.at[0, t], self.pair_sems.at[1, t], *sibling()) for t in range(Z)]

    def copy(self, src, number, z):
        slot = self.others.at[number] if number < 2 else self.relay.at[number - 2]
        return remote(src, slot, self.z_sems.at[0, number], self.z_sems.at[1, number], self.rep, z, self.core)

    def ends_copies(self):
        z, near = self.z, self.near
        return [self.copy(self.sums.at[t], number, near) for number, t in ((2, 3 - z), (3, 3 - near), (0, near))]

    def direct(self):
        return self.copy(self.sums.at[self.outer], 0, self.outer)

    def onwards(self, i):
        return self.copy(self.onward.at[i], 1, 3 - self.outer) if i == 0 else self.copy2()

    def copy2(self):
        return remote(self.onward.at[1], self.others.at[1], self.z_sems.at[0, 2], self.z_sems.at[1, 1], self.rep, self.inner, self.core)

    def begin(self):
        for c in self.pair():
            c.start()

    def add_pair(self):
        for c in self.pair():
            c.wait()
        for t in range(Z):
            self.sums[t] = (self.block(t, self.core)[...].astype(F32) + self.came[t].astype(F32)).astype(BF)

    def send(self):
        @pl.when(self.is_end)
        def _():
            for c in self.ends_copies():
                c.start()

        @pl.when(jnp.logical_not(self.is_end))
        def _():
            self.direct().start()

    def add_relay(self, i):
        @pl.when(jnp.logical_not(self.is_end))
        def _():
            self.copy(self.onward.at[i], 2 + i, self.near).wait_recv()
            to = 3 - self.outer if i == 0 else self.inner
            self.onward[i] = (self.sums[to].astype(F32) + self.relay[i].astype(F32)).astype(BF)

    def send_relay(self, i):
        @pl.when(jnp.logical_not(self.is_end))
        def _():
            self.onwards(i).start()

    def end(self):
        for i in range(2):
            self.copy(self.onward.at[i], i, self.near).wait_recv()

        @pl.when(self.is_end)
        def _():
            for c in self.ends_copies():
                c.wait_send()

        @pl.when(jnp.logical_not(self.is_end))
        def _():
            self.direct().wait_send()
            for i in range(2):
                self.onwards(i).wait_send()

        total = self.sums[self.z].astype(F32) + self.others[0].astype(F32) + self.others[1].astype(F32)
        return total.astype(BF)


ORDER = (2, 1, 3)


def forward_kernel(
    tiles, h_ref, gates, ups, downs, next_gates, next_ups, next_downs,
    o_ref, w1_ref, w2_ref, next_w1_ref, next_w2_ref, v1_ref, v2_ref, p_ref, out_sems, *scratch,
):
    half = len(scratch) // 2
    now = Gather(gates, ups, downs, v1_ref, v2_ref, scratch[0], scratch[1:half])
    later = Gather(next_gates, next_ups, next_downs, next_w1_ref, next_w2_ref, scratch[half], scratch[half + 1 :])
    step = pl.program_id(0)
    w1, w2 = now.only(0), now.only(1)
    next_w1, next_w2 = later.only(0), later.only(1)
    out = [pltpu.make_async_copy(v, w, out_sems.at[i]) for i, (v, w) in enumerate(((v1_ref, w1_ref), (v2_ref, w2_ref)))]

    @pl.when(step == 0)
    def _():
        now.join()
        meet(z_peers() + rep_peers() + [sibling()])
        w1.begin()
        w2.begin()
        later.join()
        for i in ORDER:
            w1.hand_on(i)
        next_w1.begin()
        for i in ORDER:
            w2.hand_on(i)
        for i in ORDER:
            w1.pass_in(i)
        next_w2.begin()
        w1.arrived()
        out[0].start()

    def each(do):
        for i in ORDER:
            do(i)

    for at, do in (
        (1, lambda: [each(w2.pass_in), each(next_w1.hand_on)]), (2, lambda: each(next_w2.hand_on)),
        (tiles, lambda: [w2.arrived(), out[1].start()]), (tiles + 2, lambda: each(next_w1.pass_in)),
    ):
        pl.when(step == at)(lambda do=do: do() and None)

    ff = v2_ref.shape[0]
    rows_of = pl.ds(pl.multiple_of(step % tiles * TM, TM), TM)

    @pl.when(step < tiles)
    def _():
        wide = h_ref[...].astype(F32)
        a = (wide * scale_of(wide)).astype(BF)
        for s, w in chunks(ff):
            gu = dot(a, v1_ref[:, 2 * s : 2 * (s + w)])
            gate, up = gu[:, :w], gu[:, w:]
            p_ref[rows_of, s : s + w] = (gate * sigmoid(gate) * up).astype(BF)

    @pl.when(step >= tiles)
    def _():
        o_ref[...] = h_ref[...] + dot(p_ref[rows_of, :], v2_ref[...]).astype(BF)

    @pl.when(step == 2 * tiles - 1)
    def _():
        each(next_w2.pass_in)
        later.arrived()
        now.sent()
        later.sent()
        for c in out:
            c.wait()


def backward_kernel(tiles, kept, h_ref, by_ref, w1_ref, w2_ref, *refs):
    others, (o_ref, *grads, dgu_ref, at_ref, p_ref, acc_ref, dw1_ref, dw2_ref), scratch = refs[:kept], refs[kept : kept + 10], refs[kept + 10 :]
    dgate_ref, dup_ref, ddown_ref = (g.at[0] for g in grads)
    ff = w2_ref.shape[0]
    parts = halves(ff)
    runs = [[c for c in chunks(ff) if lo <= c[0] < hi] for lo, hi in parts]
    s1, s2, s3, s4, count = marks(tiles, ff)
    step = pl.program_id(0)
    n = Scatter.SCRATCH
    first, second = (
        Scatter(dw1_ref.at[:, 2 * lo : 2 * hi], *scratch[n * k : n * (k + 1)]) for k, (lo, hi) in enumerate(parts)
    )
    down = Scatter(dw2_ref, *scratch[2 * n :])
    before = [
        (s2, first.begin), (s2 + 1, first.send), (s2 + 3, lambda: first.send_relay(0)), (s3, lambda: first.send_relay(1)),
        (s3, down.begin), (s3 + 1, down.send), (s4, lambda: down.send_relay(0)), (s4 + 1, lambda: down.send_relay(1)),
        (s4, second.begin), (s4 + 1, second.send), (s4 + 3, lambda: second.send_relay(0)),
    ]
    after = [
        (s2, first.add_pair), (s2 + 2, lambda: first.add_relay(0)), (s2 + 3, lambda: first.add_relay(1)),
        (s3, down.add_pair), (s4 - 1, lambda: down.add_relay(0)), (s4, lambda: down.add_relay(1)),
        (s4, second.add_pair), (s4 + 2, lambda: second.add_relay(0)),
    ]

    def first_end():
        put(first.end(), runs[0])

    def put(block, of):
        start = 2 * of[0][0]
        for s, w in of:
            at = 2 * s - start
            dgate_ref[:, s : s + w] = block[:, at : at + w]
            dup_ref[:, s : s + w] = block[:, at + w : at + 2 * w]

    before.append((s4, first_end))
    pl.when(step == 0)(lambda: meet(z_peers() + [sibling()]))

    @pl.when(step == 1)
    def _():
        for other, grad in zip(others, grads):
            grad[1:] = other[...]

    for at, do in before:
        pl.when(step == at)(do)

    def hidden(part, tile):
        rows_of = pl.ds(pl.multiple_of(tile * TM, TM), TM)
        wide = h_ref[...].astype(F32)
        a = (wide * scale_of(wide)).astype(BF)
        if part == 0:
            at_ref[:, rows_of] = a.T
        by = by_ref[...]
        lo, hi = parts[part]
        for s, w in runs[part]:
            gu = dot(a, w1_ref[:, 2 * s : 2 * (s + w)])
            dp = dot_nt(by, w2_ref[s : s + w, :]).astype(BF).astype(F32)
            gate, up = gu[:, :w], gu[:, w:]
            sg = sigmoid(gate)
            silu = gate * sg
            p_ref[:, s - lo : s - lo + w] = (silu * up).astype(BF)
            dgu_ref[rows_of, 2 * s : 2 * s + w] = (dp * up * (sg + silu * (1 - sg))).astype(BF)
            dgu_ref[rows_of, 2 * s + w : 2 * (s + w)] = (dp * silu).astype(BF)
        term = dot(by.T, p_ref[:, : hi - lo])

        @pl.when(tile == 0)
        def _():
            acc_ref[:, lo:hi] = term

        @pl.when(tile > 0)
        def _():
            acc_ref[:, lo:hi] += term

        if part == 1:

            @pl.when(tile == tiles - 1)
            def _():
                dw2_ref[...] = acc_ref[...].astype(BF).T

    pl.when(step < s1)(lambda: hidden(0, step))
    pl.when((step >= s2) & (step < s3))(lambda: hidden(1, step - s2))

    def weights(number):
        columns = pl.ds(pl.multiple_of(number * 256, 256), 256)
        dw1_ref[:, columns] = dot(at_ref[...], dgu_ref[:, columns]).astype(BF)

    pl.when(((step >= s1) & (step < s2)) | ((step >= s3) & (step < s4)))(
        lambda: weights(jnp.where(step < s2, step - s1, step - s3 + s2 - s1))
    )

    @pl.when(step >= s4)
    def _():
        rows_of = pl.ds(pl.multiple_of((step - s4) * TM, TM), TM)
        da = dot_nt(dgu_ref[rows_of, :], w1_ref[...]).astype(BF).astype(F32)
        wide = h_ref[...].astype(F32)
        scale = scale_of(wide)
        inner = jnp.mean(da * wide, -1, keepdims=True)
        o_ref[...] = by_ref[...] + (scale * da - (scale * scale * scale * inner) * wide).astype(BF)

    for at, do in after:
        pl.when(step == at)(do)

    @pl.when(step == count - 1)
    def _():
        second.add_relay(1)
        ddown_ref[...] = down.end()
        second.send_relay(1)
        put(second.end(), runs[1])


def halves(ff):
    cut = chunks(ff)[(len(chunks(ff)) + 1) // 2][0]
    return (0, cut), (cut, ff)


def marks(tiles, ff):
    (_, cut), _ = halves(ff)
    a, b = 2 * cut // 256, 2 * (ff - cut) // 256
    return tiles, tiles + a, 2 * tiles + a, 2 * tiles + a + b, 3 * tiles + a + b


def params(number=None):
    more = {} if number is None else {"collective_id": number, "has_side_effects": True}
    return pltpu.CompilerParams(dimension_semantics=("arbitrary",), vmem_limit_bytes=VMEM_LIMIT, **more)


def cost(flops, nbytes):
    return pl.CostEstimate(flops=flops, bytes_accessed=nbytes, transcendentals=0)


def whole(shape):
    return pl.BlockSpec(shape, lambda i: (0,) * len(shape))


def rows(width):
    return pl.BlockSpec((TM, width), lambda i: (i, 0))


def of_layer(t, n):
    return pl.BlockSpec((1, *t.shape[1:]), lambda i: (n, 0, 0))


ANY = pl.BlockSpec(memory_space=pl.ANY)


def shapes(*all_of):
    return [jax.ShapeDtypeStruct(s, BF) for s in all_of]


def forward(h, blocks, number):
    t, d = h.shape
    (_, r1, ff), r2 = blocks[0].shape, blocks[2].shape[1]
    tiles = t // TM
    w1, w2 = (8 * r1, 2 * ff), (8 * r2, d)
    return pl.pallas_call(
        functools.partial(forward_kernel, tiles), grid=(2 * tiles,), name="forward",
        in_specs=[pl.BlockSpec((TM, d), lambda i: (i % tiles, 0)), *(of_layer(b, n) for n in range(2) for b in blocks)],
        out_specs=[pl.BlockSpec((TM, d), lambda i: (jnp.maximum(i - tiles, 0), 0)), ANY, ANY, ANY, ANY],
        out_shape=shapes((t, d), w1, w2, w1, w2),
        scratch_shapes=[
            pltpu.VMEM(w1, BF), pltpu.VMEM(w2, BF), pltpu.VMEM((t, ff), BF), pltpu.SemaphoreType.DMA((2,)),
            *Gather.scratch(r1, 2 * ff), *Gather.scratch(r1, 2 * ff),
        ],
        compiler_params=params(number), cost_estimate=cost(6 * t * d * ff, 4 * t * d),
    )(h, *blocks, *blocks)


def once(shape):
    return pl.BlockSpec(shape, lambda i: (0,) * len(shape), pipeline_mode=pl.Buffered(buffer_count=1))


def backward(h, by, w1, w2, number, others=()):
    t, d = h.shape
    ff = w2.shape[0]
    tiles = t // TM
    s1, s2, s3, s4, count = marks(tiles, ff)

    def tile(i):
        return jnp.where(i < s1, i, jnp.where(i < s2, 0, jnp.where(i < s3, i - s2, jnp.where(i < s4, 0, i - s4)))), 0

    r1, r2 = d // 8, ff // 8
    (_, cut), _ = halves(ff)
    count_of = 1 + sum(t.shape[0] for t in others[:1])
    blocks = [(count_of, r1, ff), (count_of, r1, ff), (count_of, r2, d)]
    return pl.pallas_call(
        functools.partial(backward_kernel, tiles, len(others)), grid=(count,), name="backward",
        in_specs=[pl.BlockSpec((TM, d), tile), pl.BlockSpec((TM, d), tile), once(w1.shape), once(w2.shape), *(once(t.shape) for t in others)],
        out_specs=[pl.BlockSpec((TM, d), lambda i: (jnp.maximum(i - s4, 0), 0)), *(once(b) for b in blocks)],
        out_shape=shapes((t, d), *blocks),
        scratch_shapes=[
            pltpu.VMEM((t, 2 * ff), BF), pltpu.VMEM((d, t), BF), pltpu.VMEM((TM, cut), BF), pltpu.VMEM((d, ff), F32),
            pltpu.VMEM((d, 2 * ff), BF), pltpu.VMEM((ff, d), BF),
            *Scatter.scratch(r1, 2 * cut), *Scatter.scratch(r1, 2 * (ff - cut)), *Scatter.scratch(r2, d),
        ],
        compiler_params=params(number), cost_estimate=cost(16 * t * d * ff, 10**7),
    )(h, by, w1, w2, *others)


def solution(mesh):
    def step(x, dy, w_gate, w_up, w_down):
        x, by = x[0], dy[0]
        blocks = (w_gate, w_up, w_down)
        h, w1, w2, v1, v2 = forward(x, blocks, 1)
        by, *last = backward(h, by, v1, v2, 2)
        by, *both = backward(x, by, w1, w2, 3, last)
        return (by[None], *both)

    spread, by_rows = P(("rep", "dp"), None, None), P(None, "dp", None)
    group = P("rep", "dp", None)
    return jax.shard_map(
        step, mesh=mesh, in_specs=(spread, spread, by_rows, by_rows, by_rows),
        out_specs=(spread, group, group, group), check_vma=False,
    )
```
